32 devices in a mesh: grp: 8 (over z, x), neg: 4 (over y, core).
Axes of the slice: x: 2, y: 2, z: 4, core: 2. Of those that a mesh axis runs over, the one named last changes fastest.
Arguments:
- actions: bfloat16 [256, 64, 1024], P(('grp', 'neg')), may hold values from -6 to 6
- item_ids: int32 [256, 64], P(('grp', 'neg')), may hold values from 0 to 65535
- lengths: int32 [256], P(('grp', 'neg')), may hold values from 1 to 64, as said below
- owners: int32 [256], P(('grp', 'neg')), may hold values from 0 to 7, as said below
- neg_rows: int32 [2048], P(('grp', 'neg')), may hold values from 0 to 511, as said below
- w_proj: bfloat16 [1024, 4096], replicated, may hold values from -0.1875 to 0.1875
- w_out: bfloat16 [1024, 1024], replicated, may hold values from -0.1875 to 0.1875
Outputs:
- grad_actions: bfloat16 [256, 64, 1024], P(('grp', 'neg'))
- token_loss: bfloat16 [256, 64], P(('grp', 'neg'))
The draws below stay inside these ranges and needn't reach their ends.
Inputs may be any that keep to these rules, and one draw needn't show every extreme that they name: `lengths`: every history has at least one action; in every draw some history has exactly 64. `owners`: A device names each grp index as owner of exactly 1 of its histories. The histories that the device (o, c) computes (those of the devices (g, c) with owner o) hold at most 192 actions together, and in every draw some owner in every neg column computes exactly 192. `neg_rows`: each entry is h * 64 + t with t below lengths of the device's history slot h.
All inputs are finite; a program needn't handle non-finite values.
Results may differ from the reference program's by a relative error of at most 0.013.
Values may be sent and summed in bfloat16 or wider, within the bound.
No kernel may reach another device: no remote copies, remote signals or barrier semaphores. Data moves between devices by JAX's collectives and lax.ppermute only.
A program may use at most 128 MiB of HBM per device.

```python
import jax
import jax.numpy as jnp
from jax import lax

D = 1024
HEADS = 8
LMAX = 64
HIST_PAIR = 1
NEG_DEV = 64
ITEMS = 65536
HD = 1024
HIST = 8
USERS = 256
PACK = 192
POOL = 256
N_GRP = 8
N_NEG = 4


def history_plan(key):
    groups = N_GRP
    columns = N_NEG
    per_pair = HIST_PAIR
    slot_count = groups * per_pair
    subkeys = [jax.random.fold_in(key, 7100 + position) for position in range(6)]
    source_scale = jnp.left_shift(jnp.ones((columns, groups), jnp.int32), jax.random.randint(subkeys[0], (columns, groups), 0, 4))
    weights = jax.random.randint(subkeys[1], (columns, groups, groups, per_pair), 1, 5) * source_scale[:, None, :, None]
    weights = weights.reshape(columns, groups, slot_count)
    totals = jax.random.randint(subkeys[2], (columns, groups), PACK * 3 // 4, PACK + 1)
    fullest = jax.random.randint(subkeys[3], (columns, 1), 0, groups)
    totals = jnp.where(jnp.arange(groups)[None, :] == fullest, PACK, totals)
    longest = jax.random.randint(subkeys[4], (columns, groups, 1), 0, slot_count)
    is_long = jnp.arange(slot_count)[None, None, :] == longest
    others = jnp.where(is_long, 0, weights)
    spare = totals - LMAX - (slot_count - 1)
    base = 1 + spare[:, :, None] * others // jnp.sum(others, -1, keepdims=True)
    base = jnp.where(is_long, 0, jnp.minimum(base, LMAX))
    remain = totals - LMAX - jnp.sum(base, -1)
    room = jnp.where(is_long, 0, LMAX - base)
    before = jnp.cumsum(room, -1) - room
    extra = jnp.clip(remain[:, :, None] - before, 0, room)
    sizes = jnp.where(is_long, LMAX, base + extra)
    sizes = sizes.reshape(columns, groups, groups, per_pair).transpose(0, 2, 1, 3).reshape(columns, groups, slot_count)
    shuffles = jax.vmap(lambda subkey: jax.random.permutation(subkey, slot_count))(jax.random.split(subkeys[5], columns * groups))
    shuffles = shuffles.reshape(columns, groups, slot_count).astype(jnp.int32)
    history_len = jnp.take_along_axis(sizes, shuffles, -1)
    owner_index = shuffles // per_pair
    history_len = history_len.transpose(1, 0, 2).reshape(-1).astype(jnp.int32)
    owner_index = owner_index.transpose(1, 0, 2).reshape(-1).astype(jnp.int32)
    return (history_len, owner_index)


def item_plan(key):
    id_shape = (N_GRP * N_NEG * N_GRP * HIST_PAIR, LMAX)
    top_bits = ITEMS.bit_length() - 1
    levels = jax.random.randint(jax.random.fold_in(key, 7201), id_shape, 1, top_bits + 1)
    raw_ids = jax.random.randint(jax.random.fold_in(key, 7202), id_shape, 0, ITEMS)
    raw_ids = raw_ids % jnp.left_shift(jnp.ones(id_shape, jnp.int32), levels)
    offset = jax.random.randint(jax.random.fold_in(key, 7203), (), 0, ITEMS)
    return ((raw_ids * 4099 + offset) % ITEMS).astype(jnp.int32)


def draw_actions(key, part):
    item_rows = item_plan(key)
    table = jax.random.normal(jax.random.fold_in(key, 7301), (ITEMS, D), jnp.float32)
    jitter = jax.random.normal(jax.random.fold_in(key, 7302), item_rows.shape + (D,), jnp.float32)
    mixed_rows = 0.8 * table[item_rows] + 0.6 * jitter
    return jnp.clip(mixed_rows, -6.0, 6.0).astype(jnp.bfloat16)


def draw_item_ids(key, part):
    return item_plan(key)


def draw_lengths(key, part):
    return history_plan(key)[0]


def draw_owners(key, part):
    return history_plan(key)[1]


def draw_neg_rows(key, part):
    history_len = history_plan(key)[0]
    devices = N_GRP * N_NEG
    slot_count = N_GRP * HIST_PAIR
    per_device = history_len.reshape(devices, slot_count)
    chosen = jax.random.randint(jax.random.fold_in(key, 7401), (devices, NEG_DEV), 0, slot_count)
    chosen_len = jnp.take_along_axis(per_device, chosen, 1)
    within = jax.random.randint(jax.random.fold_in(key, 7402), (devices, NEG_DEV), 0, 1048576) % chosen_len
    return (chosen * LMAX + within).reshape(-1).astype(jnp.int32)


def normal_values(rng, extent, scale, bound, held_as=jnp.bfloat16):
    result = scale * jax.random.normal(rng, extent, jnp.float32)
    return jnp.clip(result, min=-bound, max=bound).astype(held_as)


def setup_inputs(seed: int = 0) -> dict:
    keys = jax.random.split(jax.random.key(seed), 8)
    return {
        "actions": draw_actions(jax.random.fold_in(keys[7], 71), 0),
        "item_ids": draw_item_ids(jax.random.fold_in(keys[7], 71), 0),
        "lengths": draw_lengths(jax.random.fold_in(keys[7], 71), 0),
        "owners": draw_owners(jax.random.fold_in(keys[7], 71), 0),
        "neg_rows": draw_neg_rows(jax.random.fold_in(keys[7], 71), 0),
        "w_proj": normal_values(keys[5], (D, 4 * HD), D ** -0.5, 0.1875),
        "w_out": normal_values(keys[6], (HD, D), HD ** -0.5, 0.1875),
    }


SOFTMAX_TEMP_SCALE = 0.05

def layer_norm(values_in):
    row_mean = lax.optimization_barrier(jnp.mean(values_in, -1, keepdims=True))
    centered = values_in - row_mean
    return centered * lax.rsqrt(lax.optimization_barrier(jnp.mean(centered * centered, -1, keepdims=True)) + 1e-05)

def unit_rows(matrix):
    return matrix * lax.rsqrt(lax.optimization_barrier(jnp.sum(matrix * matrix, -1, keepdims=True)) + 1e-06)

def unit_back(matrix, cotangent):
    inverse = lax.rsqrt(lax.optimization_barrier(jnp.sum(matrix * matrix, -1, keepdims=True)) + 1e-06)
    return inverse * cotangent - matrix * (inverse * inverse * inverse) * lax.optimization_barrier(jnp.sum(matrix * cotangent, -1, keepdims=True))

def layout(recv_len, history_cap, capacity):
    slot_count = recv_len.shape[0]
    starts = (jnp.cumsum(recv_len) - recv_len).astype(jnp.int32)
    row_index = jnp.arange(capacity, dtype=jnp.int32)
    owner_slot = lax.optimization_barrier(jnp.sum((starts[None, :] <= row_index[:, None]).astype(jnp.int32), 1)) - 1
    chosen = owner_slot[:, None] == jnp.arange(slot_count, dtype=jnp.int32)[None, :]
    row_start = lax.optimization_barrier(jnp.sum(jnp.where(chosen, starts[None, :], 0), 1)).astype(jnp.int32)
    row_len = lax.optimization_barrier(jnp.sum(jnp.where(chosen, recv_len[None, :], 0), 1)).astype(jnp.int32)
    offset = row_index - row_start
    is_live = row_index < jnp.sum(recv_len)
    gather_rows = jnp.where(is_live, owner_slot * history_cap + offset, 0).astype(jnp.int32)
    scored = is_live & (offset < row_len - 1)
    places = jnp.arange(history_cap, dtype=jnp.int32)
    inside = places[None, :] < recv_len[:, None]
    scatter_rows = jnp.where(inside, starts[:, None] + places[None, :], capacity).reshape(-1).astype(jnp.int32)
    return (gather_rows, scatter_rows, scored, inside)

def hstu_layer(xfloat, w_proj, w_out, gather_rows, scatter_rows, inside):
    slot_count, history_cap = inside.shape
    head_width = w_out.shape[0]
    head_size = head_width // HEADS
    normed = layer_norm(xfloat).astype(jnp.bfloat16)
    projected = jax.nn.silu(jnp.dot(normed, w_proj, preferred_element_type=jnp.float32)).astype(jnp.bfloat16)
    gate_part = projected[:, :head_width]
    remainder = jnp.concatenate([projected[:, head_width:], jnp.zeros((1, 3 * head_width), jnp.bfloat16)], 0)
    placed = remainder[scatter_rows].reshape(slot_count, history_cap, 3, HEADS, head_size)
    value_rows = placed[:, :, 0].astype(jnp.float32)
    query_rows = placed[:, :, 1].astype(jnp.float32)
    key_rows = placed[:, :, 2].astype(jnp.float32)
    scores = jnp.einsum('mihd,mjhd->mhij', query_rows, key_rows) * head_size ** (-0.5)
    causal = jnp.arange(history_cap)[:, None] >= jnp.arange(history_cap)[None, :]
    allowed = causal[None, None, :, :] & inside[:, None, None, :]
    weights = jnp.where(allowed, jax.nn.silu(scores), 0.0).astype(jnp.bfloat16)
    mixed_rows = jnp.einsum('mhij,mjhd->mihd', weights.astype(jnp.float32), value_rows)
    mixed_rows = mixed_rows.reshape(slot_count * history_cap, head_width)
    attended = layer_norm(mixed_rows[gather_rows])
    gated_rows = (attended * gate_part.astype(jnp.float32)).astype(jnp.bfloat16)
    return xfloat + jnp.dot(gated_rows, w_out, preferred_element_type=jnp.float32)

def owner_work(recv_x, recv_ids, recv_len, negative_unit_pool, pool_ids, w_proj, w_out):
    slot_count, history_cap, model_dim = recv_x.shape
    capacity = slot_count * history_cap * 3 // 8
    gather_rows, scatter_rows, scored, inside = layout(recv_len, history_cap, capacity)
    compact = recv_x.reshape(slot_count * history_cap, model_dim)[gather_rows].astype(jnp.float32)
    compact_ids = recv_ids.reshape(-1)[gather_rows]

    def forward(xfloat):
        return hstu_layer(xfloat, w_proj, w_out, gather_rows, scatter_rows, inside)
    output, pull_back = jax.vjp(forward, compact)
    target = jnp.roll(compact, -1, 0)
    target_ids = jnp.roll(compact_ids, -1, 0)
    output_unit_vector = unit_rows(output)
    output_lowrank = output_unit_vector.astype(jnp.bfloat16)
    target_unit_vector = unit_rows(target)
    positive_score = lax.optimization_barrier(jnp.sum(output_unit_vector * target_unit_vector, -1)) / SOFTMAX_TEMP_SCALE
    logit_scores = lax.dot_general(output_lowrank, negative_unit_pool, (((1,), (1,)), ((), ())), preferred_element_type=jnp.float32) / SOFTMAX_TEMP_SCALE
    kept_mask = scored[:, None] & (pool_ids[None, :] != target_ids[:, None])
    others = jnp.where(kept_mask, jnp.exp(logit_scores), 0.0)
    own_term = jnp.exp(positive_score)
    totals = own_term + lax.optimization_barrier(jnp.sum(others, 1))
    token_loss = jnp.where(scored, jnp.log(totals) - positive_score, 0.0)
    softmax_probs = (others / totals[:, None]).astype(jnp.bfloat16)
    leading_gradient = jnp.where(scored, own_term / totals - 1.0, 0.0)
    unit_vector_gradient = (jnp.dot(softmax_probs, negative_unit_pool, preferred_element_type=jnp.float32) + leading_gradient[:, None] * target_unit_vector) / SOFTMAX_TEMP_SCALE
    target_gradient = leading_gradient[:, None] * output_unit_vector / SOFTMAX_TEMP_SCALE
    grad_output = unit_back(output, unit_vector_gradient)
    grad_rows = pull_back(grad_output)[0] + jnp.roll(unit_back(target, target_gradient), 1, 0)
    back_x = jnp.concatenate([grad_rows.astype(jnp.bfloat16), jnp.zeros((1, model_dim), jnp.bfloat16)], 0)[scatter_rows]
    back_loss = jnp.concatenate([token_loss.astype(jnp.bfloat16), jnp.zeros((1,), jnp.bfloat16)], 0)[scatter_rows]
    return (back_x.reshape(slot_count, history_cap, model_dim), back_loss.reshape(slot_count, history_cap), output_lowrank, softmax_probs)

def reference(actions, item_ids, lengths, owners, neg_rows, w_proj, w_out):
    groups = N_GRP
    columns = N_NEG
    acts = actions.reshape(groups, columns, HIST, LMAX, D)
    idents = item_ids.reshape(groups, columns, HIST, LMAX)
    history_len = lengths.reshape(groups, columns, HIST)
    owning = owners.reshape(groups, columns, HIST)
    sampled = neg_rows.reshape(groups, columns, NEG_DEV)
    flat_acts = acts.reshape(groups, columns, HIST * LMAX, D)
    flat_ids = idents.reshape(groups, columns, HIST * LMAX)
    picked = jax.vmap(jax.vmap(lambda table, where_rows: table[where_rows]))(flat_acts, sampled)
    picked_ids = jax.vmap(jax.vmap(lambda table, where_rows: table[where_rows]))(flat_ids, sampled)
    pool_raw = picked.astype(jnp.float32).reshape(groups, POOL, D)
    negative_unit_pool = unit_rows(pool_raw).astype(jnp.bfloat16)
    pool_ids = picked_ids.reshape(groups, POOL)
    flat_index = jnp.arange(groups * HIST, dtype=jnp.int32)

    def column_work(carry, column):
        col_acts = acts[:, column].reshape(groups * HIST, LMAX, D)
        col_ids = idents[:, column].reshape(groups * HIST, LMAX)
        col_len = history_len[:, column].reshape(groups * HIST)
        owner_key = owning[:, column].reshape(groups * HIST)
        ordering = jnp.argsort(owner_key * (groups * HIST) + flat_index).astype(jnp.int32)
        chosen = ordering.reshape(groups, HIST)

        def per_owner(item):
            picks, owner_id = item
            back_x, back_loss, output_lowrank, softmax_probs = owner_work(col_acts[picks], col_ids[picks], col_len[picks], negative_unit_pool[owner_id], pool_ids[owner_id], w_proj, w_out)
            contribution_rows = lax.dot_general(softmax_probs, output_lowrank, (((0,), (0,)), ((), ())), preferred_element_type=jnp.float32) / SOFTMAX_TEMP_SCALE
            return (back_x, back_loss, contribution_rows)
        back_x, back_loss, contribution_rows = lax.map(per_owner, (chosen, jnp.arange(groups, dtype=jnp.int32)))
        grads_col = jnp.zeros((groups * HIST, LMAX, D), jnp.bfloat16).at[ordering].set(back_x.reshape(groups * HIST, LMAX, D))
        loss_col = jnp.zeros((groups * HIST, LMAX), jnp.bfloat16).at[ordering].set(back_loss.reshape(groups * HIST, LMAX))
        return (carry + contribution_rows, (grads_col, loss_col))
    sums, (grads_cols, loss_cols) = lax.scan(column_work, jnp.zeros((groups, POOL, D), jnp.float32), jnp.arange(columns, dtype=jnp.int32))
    grads_all = grads_cols.reshape(columns, groups, HIST, LMAX, D).transpose(1, 0, 2, 3, 4)
    losses_all = loss_cols.reshape(columns, groups, HIST, LMAX).transpose(1, 0, 2, 3)
    neg_grads = unit_back(pool_raw, sums).reshape(groups * columns, NEG_DEV, D)
    device_grads = grads_all.reshape(groups * columns, HIST * LMAX, D)
    device_rows = sampled.reshape(groups * columns, NEG_DEV)

    def add_negatives(item):
        grad_block, extra_rows, row_ids = item
        return grad_block.astype(jnp.float32).at[row_ids].add(extra_rows).astype(jnp.bfloat16)
    finished = lax.map(add_negatives, (device_grads, neg_grads, device_rows))
    return (finished.reshape(USERS, LMAX, D), losses_all.reshape(USERS, LMAX))
```

```python
import functools

import jax
import jax.numpy as jnp
from jax import lax
from jax.experimental import pallas as pl
from jax.experimental.pallas import tpu as pltpu
from jax.sharding import PartitionSpec as P

HEADS = 8
TEMP = 0.05
TILE = 128
BIG = 384
META = 8
AXES = ("grp", "neg")
BF = jnp.bfloat16
F32 = jnp.float32
VMEM = pltpu.VMEM
SMEM = pltpu.SMEM
ANY = pl.ANY


def dot(a, b, ca, cb):
    return lax.dot_general(a, b, (((ca,), (cb,)), ((), ())), preferred_element_type=F32)


def slot_of(owner, groups):
    return (owner % 2) * (groups // 2) + owner // 2


def owner_at(slot, groups):
    half = groups // 2
    return (slot % half) * 2 + slot // half


def my_slot(groups, columns):
    return lax.rem(lax.axis_index("grp") * columns + lax.axis_index("neg"), groups)


def meta_rows(rows, cap):
    line = lax.broadcasted_iota(jnp.int32, (META, cap), 0)
    block = jnp.zeros((META, cap), F32)
    for index, row in enumerate(rows):
        block = jnp.where(line == index, row, block)
    if cap < 128:
        block = jnp.concatenate([block, jnp.zeros((META, 128 - cap), F32)], 1)
    return block.astype(BF)


def history_at(owners_ref, owner, slots):
    found = jnp.int32(0)
    for h in range(slots):
        found = jnp.where(owners_ref[h] == owner, jnp.int32(h), found)
    return found


def pack_kernel(groups, columns, cap, owners, lengths, acts, ids, rows_line, *outs):
    hist, pool = outs[:groups], outs[groups]
    me = my_slot(groups, columns)
    for d in range(groups):
        h = history_at(owners, owner_at(me ^ d, groups), groups)
        start = pl.multiple_of(h * cap, cap)
        hist[d][0:cap, :] = acts[pl.ds(start, cap), :]
        line = ids[pl.ds(h, 1), :]
        high, low = (line >> 8).astype(F32), (line & 255).astype(F32)
        hist[d][cap : cap + META, 0:128] = meta_rows(
            [high, low, lengths[h].astype(F32)], cap
        )
    count = rows_line.shape[1]
    picks = rows_line[...]
    row = lax.broadcasted_iota(jnp.int32, (groups * cap, count), 0)
    pool[0:count, :] = dot((row == picks).astype(BF), acts[...], 0, 0).astype(BF)
    shift = cap.bit_length() - 1
    place = lax.broadcasted_iota(jnp.int32, (cap, count), 0)
    within = (place == (picks & (cap - 1))).astype(BF)
    all_ids = ids[...]
    slot = lax.broadcasted_iota(jnp.int32, (groups, count), 0) == (picks >> shift)
    parts = []
    for part in (all_ids >> 8, all_ids & 255):
        table = dot(part.astype(F32).astype(BF), within, 1, 0)
        parts.append(jnp.sum(jnp.where(slot, table, 0.0), 0, keepdims=True))
    pool[count : count + META, 0:128] = meta_rows(parts, count)


def sigmoid(x):
    return 0.5 * jnp.tanh(0.5 * x) + 0.5


def main_kernel(groups, columns, cap, count, *refs):
    hist_in = refs[:groups]
    pool_in = refs[groups : groups + columns]
    wp_hbm, wo_hbm = refs[groups + columns : groups + columns + 2]
    outs = refs[groups + columns + 2 :][: groups + columns]
    hist_out, pool_out = outs[:groups], outs[groups:]
    (
        wp, wo, stage, pstage, xs, nb, proj, dsil, mix, out, dk, gdm,
        upool, probs, tid, live, rstd, r2s, poss, wsem, hsem,
    ) = refs[2 * (groups + columns) + 2 :]
    D = xs.shape[1]
    HD = wo.shape[0]
    hs = HD // HEADS
    scale = hs ** -0.5
    pool_size = columns * count
    off = cap
    chunk = 256
    chunks = 4 * HD // chunk
    inv_temp = 1.0 / TEMP

    def wcopy(c):
        cols = pl.ds(pl.multiple_of(c * chunk, chunk), chunk)
        return pltpu.make_async_copy(wp_hbm.at[:, cols], wp.at[:, cols], wsem.at[c])

    wocopy = pltpu.make_async_copy(wo_hbm, wo, wsem.at[chunks])
    hcopies = [
        pltpu.make_async_copy(hist_in[m], stage.at[m], hsem.at[m]) for m in range(groups)
    ]
    pcopies = [
        pltpu.make_async_copy(pool_in[k], pstage.at[k], hsem.at[groups + k])
        for k in range(columns)
    ]
    for copy in hcopies:
        copy.start()
    for c in range(chunks):
        wcopy(c).start()
    for copy in pcopies:
        copy.start()
    wocopy.start()
    live[...] = jnp.zeros_like(live)
    for copy in hcopies:
        copy.wait()

    eye_r = lax.broadcasted_iota(jnp.int32, (cap, cap), 0)
    eye_c = lax.broadcasted_iota(jnp.int32, (cap, cap), 1)
    place = lax.broadcasted_iota(jnp.int32, (cap, 1), 0)
    starts, sizes = [], []
    place_now = jnp.int32(off)
    for m in range(groups):
        meta = stage[m, cap : cap + META, 0:128].astype(F32)
        n = jnp.max(meta[2:3, :]).astype(jnp.int32)
        starts.append(place_now)
        sizes.append(n)
        place_now = place_now + ((n + 15) // 16) * 16
    total = place_now - off
    tiles = (total + TILE - 1) // TILE
    bigs = (total + BIG - 1) // BIG

    for m in range(groups):
        rows = pl.ds(pl.multiple_of(starts[m], 16), cap)
        xs[rows, :] = stage[m, 0:cap, :]
        meta = stage[m, cap : cap + META, 0:128].astype(F32)
        ids = meta[0:1, 0:cap] * 256.0 + meta[1:2, 0:cap]
        nxt = jnp.sum(jnp.where(eye_c == eye_r + 1, ids, 0.0), 1, keepdims=True)
        tid[rows, :] = nxt
        live[rows, :] = jnp.where(place < sizes[m] - 1, 1.0, 0.0)
    tail = pl.ds(pl.multiple_of(place_now, 16), TILE + 16)
    xs[tail, :] = jnp.zeros((TILE + 16, D), BF)

    def tile_at(t):
        return pl.multiple_of(off + t * TILE, 64)

    def big_rows(t):
        return pl.ds(pl.multiple_of(off + t * BIG, 64), BIG)

    def each_tile(body):
        def step(t, carry):
            body(tile_at(t), pl.ds(tile_at(t), TILE))
            return carry

        lax.fori_loop(0, tiles, step, 0)

    def each_big(body, pieces):
        def step(i, carry):
            t = i // pieces
            c = i - t * pieces
            body(big_rows(t), c)
            return carry

        lax.fori_loop(0, bigs * pieces, step, 0)

    @each_tile
    def _(base, rows):
        x = xs[rows, :].astype(F32)
        mean = jnp.mean(x, 1, keepdims=True)
        centered = x - mean
        r = lax.rsqrt(jnp.mean(centered * centered, 1, keepdims=True) + 1e-5)
        nb[rows, :] = (centered * r).astype(BF)
        rstd[rows, :] = r

    def columns_at(c, width):
        return pl.ds(pl.multiple_of(c * width, width), width)

    @functools.partial(each_big, pieces=chunks)
    def _(rows, c):
        @pl.when(rows.start == off)
        def _():
            wcopy(c).wait()

        cols = columns_at(c, chunk)
        pre = dot(nb[rows, :], wp[:, cols], 1, 0)
        sg = sigmoid(pre)
        act = pre * sg
        proj[rows, cols] = act.astype(BF)
        dsil[rows, cols] = (sg + act * (1.0 - sg)).astype(BF)

    keys = TILE + cap

    def labels(pos, dead):
        label = jnp.zeros(pos.shape, jnp.int32)
        inside = jnp.zeros(pos.shape, jnp.int32)
        for m in range(groups):
            after = pos >= starts[m]
            label = label + jnp.where(after, 1, 0)
            inside = jnp.where(after & (pos < starts[m] + sizes[m]), 1, inside)
        return jnp.where(inside > 0, label, dead)

    def allowed_at(base):
        q_pos = base + lax.broadcasted_iota(jnp.int32, (TILE, 1), 0)
        k_pos = base - cap + lax.broadcasted_iota(jnp.int32, (1, keys), 1)
        return (labels(q_pos, -2) == labels(k_pos, -1)) & (k_pos <= q_pos)

    def head(ref, rows, part, e):
        return ref[rows, part * HD + e * hs : part * HD + (e + 1) * hs]

    wide0 = pl.ds(0, cap)
    proj[wide0, :] = jnp.zeros((cap, 4 * HD), BF)

    @each_tile
    def _(base, rows):
        wide = pl.ds(pl.multiple_of(base - cap, 64), keys)
        allowed = allowed_at(base)
        for e0 in range(0, HEADS, 4):
            es = range(e0, e0 + 4)
            scores = [
                dot(head(proj, rows, 2, e), head(proj, wide, 3, e), 1, 1) * scale for e in es
            ]
            ws = [jnp.where(allowed, s * sigmoid(s), 0.0).astype(BF) for s in scores]
            mixed = [dot(w, head(proj, wide, 1, e), 1, 0) for w, e in zip(ws, es)]
            for e, value in zip(es, mixed):
                mix[rows, e * hs : (e + 1) * hs] = value

    @each_tile
    def _(base, rows):
        mixed = mix[rows, :]
        centered = mixed - jnp.mean(mixed, 1, keepdims=True)
        r2 = lax.rsqrt(jnp.mean(centered * centered, 1, keepdims=True) + 1e-5)
        att = centered * r2
        mix[rows, :] = att
        r2s[rows, :] = r2
        gdm[rows, :] = (att * proj[rows, 0:HD].astype(F32)).astype(BF)

    wocopy.wait()

    @functools.partial(each_big, pieces=D // chunk)
    def _(rows, c):
        cols = columns_at(c, chunk)
        out[rows, cols] = xs[rows, cols].astype(F32) + dot(gdm[rows, :], wo[:, cols], 1, 0)

    def target_rows(base):
        ext = xs[pl.ds(base, TILE + 16), :].astype(F32)
        tgt = pltpu.roll(ext, TILE + 15, 0)[0:TILE, :]
        return tgt, lax.rsqrt(jnp.sum(tgt * tgt, 1, keepdims=True) + 1e-6)

    @each_tile
    def _(base, rows):
        o = out[rows, :]
        ro = lax.rsqrt(jnp.sum(o * o, 1, keepdims=True) + 1e-6)
        gdm[rows, :] = (o * ro).astype(BF)
        tgt, rt = target_rows(base)
        poss[rows, :] = jnp.sum(o * tgt, 1, keepdims=True) * ro * rt

    for copy in pcopies:
        copy.wait()
    pool_ids = []
    for k in range(columns):
        raw = pstage[k, 0:count, :].astype(F32)
        inv = lax.rsqrt(jnp.sum(raw * raw, 1, keepdims=True) + 1e-6)
        upool[k * count : (k + 1) * count, :] = (raw * inv).astype(BF)
        meta = pstage[k, count : count + META, 0:128].astype(F32)
        pool_ids.append(meta[0:1, 0:count] * 256.0 + meta[1:2, 0:count])
    pool_ids = jnp.concatenate(pool_ids, 1)

    def clear(t, carry):
        gdm[pl.ds(tile_at(t), TILE), :] = jnp.zeros((TILE, D), BF)
        return carry

    lax.fori_loop(tiles, bigs * (BIG // TILE), clear, 0)
    dk[0:pool_size, :] = jnp.zeros((pool_size, D), F32)

    @functools.partial(each_big, pieces=1)
    def _(rows, c):
        low = gdm[rows, :]
        logits = dot(low, upool[...], 1, 1) * inv_temp
        scored = live[rows, :] > 0.5
        kept = scored & (pool_ids != tid[rows, :])
        others = jnp.where(kept, jnp.exp(logits), 0.0)
        pos = poss[rows, :] * inv_temp
        own = jnp.exp(pos)
        totals = own + jnp.sum(others, 1, keepdims=True)
        tid[rows, :] = jnp.where(scored, jnp.log(totals) - pos, 0.0)
        live[rows, :] = jnp.where(scored, (own / totals - 1.0) * inv_temp, 0.0)
        prob = jnp.where(kept, others / totals, 0.0).astype(BF)
        probs[rows, :] = prob
        dk[0:pool_size, :] += dot(prob, low, 0, 0)

    for k in range(columns):
        part = dk[k * count : (k + 1) * count, :] * inv_temp
        pstage[k, 0:count, :] = part.astype(BF)
        pcopies[k] = pltpu.make_async_copy(
            pstage.at[k, pl.ds(0, count), :], pool_out[k], hsem.at[groups + k]
        )
        pcopies[k].start()

    @each_tile
    def _(base, rows):
        o, coef = out[rows, :], live[rows, :]
        ro = lax.rsqrt(jnp.sum(o * o, 1, keepdims=True) + 1e-6)
        tgt, rt = target_rows(base)
        gu = dot(probs[rows, :], upool[...], 1, 0) * inv_temp + (coef * rt) * tgt
        og = jnp.sum(o * gu, 1, keepdims=True)
        gout = ro * gu - o * (ro * ro * ro * og)
        out[rows, :] = gout
        gdm[rows, :] = gout.astype(BF)
        cosine = poss[rows, :]
        xs[rows, :] = (
            (rt * coef * ro) * o - tgt * (rt * rt * coef * cosine)
        ).astype(BF)

    @functools.partial(each_big, pieces=HD // chunk)
    def _(rows, c):
        dk[rows, columns_at(c, chunk)] = dot(gdm[rows, :], wo[columns_at(c, chunk), :], 1, 1)

    gdm[wide0, :] = jnp.zeros((cap, HD), BF)

    @each_tile
    def _(base, rows):
        dg, att = dk[rows, :], mix[rows, :]
        dsil[rows, 0:HD] = (dg * att * dsil[rows, 0:HD].astype(F32)).astype(BF)
        da = dg * proj[rows, 0:HD].astype(F32)
        mean_a = jnp.mean(da, 1, keepdims=True)
        mean_b = jnp.mean(da * att, 1, keepdims=True)
        gdm[rows, :] = (r2s[rows, :] * (da - mean_a - att * mean_b)).astype(BF)

    @each_tile
    def _(base, rows):
        low_half = pl.ds(pl.multiple_of(base - cap, 64), cap)
        wide = pl.ds(pl.multiple_of(base - cap, 64), keys)
        allowed = allowed_at(base)
        for e0 in range(0, HEADS, 2):
            es = range(e0, e0 + 2)
            scores = [
                dot(head(proj, rows, 2, e), head(proj, wide, 3, e), 1, 1) * scale for e in es
            ]
            dws = [dot(head(gdm, rows, 0, e), head(proj, wide, 1, e), 1, 1) for e in es]
            ws, dss = [], []
            for score, dw in zip(scores, dws):
                sg = sigmoid(score)
                act = score * sg
                ws.append(jnp.where(allowed, act, 0.0).astype(BF))
                slope = (sg + act * (1.0 - sg)) * scale
                dss.append(jnp.where(allowed, dw * slope, 0.0).astype(BF))
            dqs = [dot(ds, head(proj, wide, 3, e), 1, 0) for ds, e in zip(dss, es)]
            dks = [dot(ds, head(proj, rows, 2, e), 0, 0) for ds, e in zip(dss, es)]
            dvs = [dot(w, head(gdm, rows, 0, e), 0, 0) for w, e in zip(ws, es)]
            for e, dq, dkk, dv in zip(es, dqs, dks, dvs):
                cols = slice(2 * HD + e * hs, 2 * HD + (e + 1) * hs)
                dsil[rows, cols] = (dq * dsil[rows, cols].astype(F32)).astype(BF)
                cols = slice(e * hs, (e + 1) * hs)
                for ref, value in ((dk, dkk), (mix, dv)):
                    ref[low_half, cols] += value[0:cap, :]
                    ref[rows, cols] = value[cap:keys, :]

    @each_tile
    def _(base, rows):
        for part, ref in ((1, mix), (3, dk)):
            cols = slice(part * HD, (part + 1) * HD)
            dsil[rows, cols] = (ref[rows, :] * dsil[rows, cols].astype(F32)).astype(BF)

    @functools.partial(each_big, pieces=D // chunk)
    def _(rows, c):
        mix[rows, columns_at(c, chunk)] = dot(dsil[rows, :], wp[columns_at(c, chunk), :], 1, 1)

    @each_tile
    def _(base, rows):
        dn, n = mix[rows, :], nb[rows, :].astype(F32)
        mean_a = jnp.mean(dn, 1, keepdims=True)
        mean_b = jnp.mean(dn * n, 1, keepdims=True)
        out[rows, :] = out[rows, :] + rstd[rows, :] * (dn - mean_a - n * mean_b)

    ocopies = []
    for m in range(groups):
        rows = pl.ds(pl.multiple_of(starts[m], 16), cap)
        nxt = pltpu.roll(xs[rows, :].astype(F32), 1, 0)
        grad = out[rows, :] + jnp.where(place == 0, 0.0, nxt)
        stage[m, 0:cap, :] = jnp.where(place < sizes[m], grad, 0.0).astype(BF)
        column = jnp.where(place < sizes[m], tid[rows, :], 0.0)
        line = jnp.sum(jnp.where(eye_c == eye_r, column, 0.0), 0, keepdims=True)
        stage[m, cap : cap + META, 0:128] = meta_rows([line], cap)
        ocopies.append(pltpu.make_async_copy(stage.at[m], hist_out[m], hsem.at[m]))
        ocopies[-1].start()
    for copy in ocopies + pcopies:
        copy.wait()


def final_kernel(groups, columns, cap, count, owners, rows_line, *refs):
    hist = refs[:groups]
    pools = refs[groups : groups + columns]
    picked = refs[groups + columns]
    grad_out, loss_out = refs[groups + columns + 1 :]
    me = my_slot(groups, columns)
    total = pools[0][...].astype(F32)
    for k in range(1, columns):
        total = total + pools[k][...].astype(F32)
    raw = picked[0:count, :].astype(F32)
    inv = lax.rsqrt(jnp.sum(raw * raw, 1, keepdims=True) + 1e-6)
    own = inv * total - raw * (
        inv * inv * inv * jnp.sum(raw * total, 1, keepdims=True)
    )
    high = own.astype(BF)
    low = (own - high.astype(F32)).astype(BF)
    picks = rows_line[...]
    row = lax.broadcasted_iota(jnp.int32, (cap, count), 0)
    line = lax.broadcasted_iota(jnp.int32, (groups, cap), 0)
    losses = jnp.zeros((groups, cap), F32)
    for d in range(groups):
        h = history_at(owners, owner_at(me ^ d, groups), groups)
        start = pl.multiple_of(h * cap, cap)
        chosen = (row + start == picks).astype(BF)
        extra = dot(chosen, high, 1, 0) + dot(chosen, low, 1, 0)
        grad_out[pl.ds(start, cap), :] = (hist[d][0:cap, :].astype(F32) + extra).astype(BF)
        meta = hist[d][cap : cap + META, 0:128].astype(F32)
        losses = jnp.where(line == h, meta[0:1, 0:cap], losses)
    loss_out[...] = losses.astype(BF)


def spec(space):
    return pl.BlockSpec(memory_space=space)


def shape(*dims):
    return jax.ShapeDtypeStruct(dims, BF)


def per_device(actions, item_ids, lengths, owners, neg_rows, w_proj, w_out):
    slots, cap, D = actions.shape
    groups, columns = lax.axis_size("grp"), lax.axis_size("neg")
    count = neg_rows.shape[0]
    HD = w_out.shape[0]
    assert slots == groups
    flat = actions.reshape(slots * cap, D)
    rows_line = neg_rows.reshape(1, count)

    packed = pl.pallas_call(
        functools.partial(pack_kernel, groups, columns, cap),
        out_shape=[shape(cap + META, D)] * groups + [shape(count + META, D)],
        in_specs=[spec(SMEM)] * 2 + [spec(VMEM)] * 3,
        out_specs=[spec(VMEM)] * (groups + 1),
        name="pack",
    )(owners, lengths, flat, item_ids, rows_line)
    hist, picked = packed[:groups], packed[groups]

    def xor_pairs(d):
        return [
            (b * groups + p, b * groups + (p ^ d))
            for b in range(columns)
            for p in range(groups)
        ]

    def pool_pairs(k):
        return [
            (o * columns + n, ((n + k) % columns) * groups + slot_of(o, groups))
            for o in range(groups)
            for n in range(columns)
        ]

    order = sorted(range(1, groups), key=lambda d: (-d))

    def exchange(parts):
        got = {0: parts[0]}
        for d in order:
            got[d] = lax.ppermute(parts[d], AXES, xor_pairs(d))
        return [got[d] for d in range(groups)]

    pool_got = [lax.ppermute(picked, AXES, pool_pairs(k)) for k in range(columns)]
    recv = exchange(hist)

    live_rows = groups * cap
    R = cap + max(pl.cdiv(live_rows, BIG) * BIG, live_rows + TILE + 16)
    pool_size = columns * count
    vm = pltpu.VMEM
    results = pl.pallas_call(
        functools.partial(main_kernel, groups, columns, cap, count),
        out_shape=[shape(cap + META, D)] * groups + [shape(count, D)] * columns,
        in_specs=[spec(ANY)] * (groups + columns + 2),
        out_specs=[spec(ANY)] * (groups + columns),
        scratch_shapes=[
            vm((D, 4 * HD), BF), vm((HD, D), BF),
            vm((groups, cap + META, D), BF), vm((columns, count + META, D), BF),
            vm((R, D), BF), vm((R, D), BF),
            vm((R, 4 * HD), BF), vm((R, 4 * HD), BF),
            vm((R, HD), F32), vm((R, D), F32), vm((R, HD), F32), vm((R, HD), BF),
            vm((pool_size, D), BF), vm((R, pool_size), BF),
            vm((R, 1), F32), vm((R, 1), F32), vm((R, 1), F32),
            vm((R, 1), F32), vm((R, 1), F32),
            pltpu.SemaphoreType.DMA((4 * HD // 256 + 1,)),
            pltpu.SemaphoreType.DMA((groups + columns,)),
        ],
        compiler_params=pltpu.CompilerParams(vmem_limit_bytes=67043328),
        cost_estimate=pl.CostEstimate(
            flops=10**10, bytes_accessed=15 * 10**6, transcendentals=10**6
        ),
        name="layer",
    )(*recv, *pool_got, w_proj, w_out)
    back = exchange(results[:groups])

    pool_back = [
        lax.ppermute(results[groups + k], AXES, [(b, a) for a, b in pool_pairs(k)])
        for k in range(columns)
    ]
    grads, losses = pl.pallas_call(
        functools.partial(final_kernel, groups, columns, cap, count),
        out_shape=[shape(slots * cap, D), shape(slots, cap)],
        in_specs=[spec(SMEM)] + [spec(VMEM)] * (groups + columns + 2),
        out_specs=[spec(VMEM)] * 2,
        name="finish",
    )(owners, rows_line, *back, *pool_back, picked)
    return grads.reshape(slots, cap, D), losses


def solution(mesh):
    whole = P(AXES)
    return jax.shard_map(
        per_device,
        mesh=mesh,
        in_specs=(whole,) * 5 + (P(), P()),
        out_specs=(whole, whole),
        check_vma=False,
    )
```

```python
import functools

import jax
import jax.numpy as jnp
from jax import lax
from jax.experimental import pallas as pl
from jax.experimental.pallas import tpu as pltpu
from jax.sharding import PartitionSpec as P

HEADS = 8
TEMP = 0.05
TILE = 128
BIG = 384
META = 8
AXES = ("grp", "neg")
BF = jnp.bfloat16
F32 = jnp.float32
VMEM = pltpu.VMEM
SMEM = pltpu.SMEM
ANY = pl.ANY


def dot(a, b, ca, cb):
    return lax.dot_general(a, b, (((ca,), (cb,)), ((), ())), preferred_element_type=F32)


def slot_of(owner, block, groups):
    return ((owner % 2) * (groups // 2) + owner // 2) ^ (2 * (block % 2))


def owner_at(slot, block, groups):
    slot = slot ^ (2 * lax.rem(block, 2))
    half = groups // 2
    return lax.rem(slot, half) * 2 + slot // half


def my_place(groups, columns):
    flat = lax.axis_index("grp") * columns + lax.axis_index("neg")
    return lax.div(flat, groups), lax.rem(flat, groups)


def meta_rows(rows, cap):
    line = lax.broadcasted_iota(jnp.int32, (META, cap), 0)
    block = jnp.zeros((META, cap), F32)
    for index, row in enumerate(rows):
        block = jnp.where(line == index, row, block)
    if cap < 128:
        block = jnp.concatenate([block, jnp.zeros((META, 128 - cap), F32)], 1)
    return block.astype(BF)


def history_at(owners_ref, owner, slots):
    found = jnp.int32(0)
    for h in range(slots):
        found = jnp.where(owners_ref[h] == owner, jnp.int32(h), found)
    return found


def pack_kernel(groups, columns, cap, owners, lengths, acts, ids, rows_line, *outs):
    hist, pool = outs[:groups], outs[groups]
    block, me = my_place(groups, columns)
    for d in range(groups):
        h = history_at(owners, owner_at(me ^ d, block, groups), groups)
        start = pl.multiple_of(h * cap, cap)
        hist[d][0:cap, :] = acts[pl.ds(start, cap), :]
        line = ids[pl.ds(h, 1), :]
        high, low = (line >> 8).astype(F32), (line & 255).astype(F32)
        hist[d][cap : cap + META, 0:128] = meta_rows(
            [high, low, lengths[h].astype(F32)], cap
        )
    count = rows_line.shape[1]
    picks = rows_line[...]
    row = lax.broadcasted_iota(jnp.int32, (groups * cap, count), 0)
    pool[0:count, :] = dot((row == picks).astype(BF), acts[...], 0, 0).astype(BF)
    shift = cap.bit_length() - 1
    place = lax.broadcasted_iota(jnp.int32, (cap, count), 0)
    within = (place == (picks & (cap - 1))).astype(BF)
    all_ids = ids[...]
    slot = lax.broadcasted_iota(jnp.int32, (groups, count), 0) == (picks >> shift)
    parts = []
    for part in (all_ids >> 8, all_ids & 255):
        table = dot(part.astype(F32).astype(BF), within, 1, 0)
        parts.append(jnp.sum(jnp.where(slot, table, 0.0), 0, keepdims=True))
    pool[count : count + META, 0:128] = meta_rows(parts, count)


def sigmoid(x):
    return 0.5 * jnp.tanh(0.5 * x) + 0.5


def main_kernel(groups, columns, cap, count, *refs):
    hist_in = refs[:groups]
    pool_in = refs[groups : groups + columns]
    wp_hbm, wo_hbm = refs[groups + columns : groups + columns + 2]
    outs = refs[groups + columns + 2 :][: groups + columns]
    hist_out, pool_out = outs[:groups], outs[groups:]
    (
        wp, wo, stage, pstage, xs, nb, proj, dsil, mix, out, dk, gdm,
        upool, probs, tid, live, rstd, r2s, poss, wsem, hsem,
    ) = refs[2 * (groups + columns) + 2 :]
    D = xs.shape[1]
    HD = wo.shape[0]
    hs = HD // HEADS
    scale = hs ** -0.5
    pool_size = columns * count
    off = cap
    chunk = 256
    chunks = 4 * HD // chunk
    roomy = xs.shape[0] <= 1024
    wide_step, width, back_heads = (4, D, HEADS) if roomy else (1, chunk, 2)
    inv_temp = 1.0 / TEMP

    def wcopy(c):
        cols = pl.ds(pl.multiple_of(c * chunk, chunk), chunk)
        return pltpu.make_async_copy(wp_hbm.at[:, cols], wp.at[:, cols], wsem.at[c])

    wocopy = pltpu.make_async_copy(wo_hbm, wo, wsem.at[chunks])
    hcopies = [
        pltpu.make_async_copy(hist_in[m], stage.at[m], hsem.at[m]) for m in range(groups)
    ]
    pcopies = [
        pltpu.make_async_copy(pool_in[k], pstage.at[k], hsem.at[groups + k])
        for k in range(columns)
    ]
    for copy in hcopies:
        copy.start()
    for c in range(chunks):
        wcopy(c).start()
    for copy in pcopies:
        copy.start()
    wocopy.start()
    live[...] = jnp.zeros_like(live)
    for copy in hcopies:
        copy.wait()

    eye_r = lax.broadcasted_iota(jnp.int32, (cap, cap), 0)
    eye_c = lax.broadcasted_iota(jnp.int32, (cap, cap), 1)
    place = lax.broadcasted_iota(jnp.int32, (cap, 1), 0)
    starts, sizes = [], []
    place_now = jnp.int32(off)
    for m in range(groups):
        meta = stage[m, cap : cap + META, 0:128].astype(F32)
        n = jnp.max(meta[2:3, :]).astype(jnp.int32)
        starts.append(place_now)
        sizes.append(n)
        place_now = place_now + ((n + 15) // 16) * 16
    total = place_now - off
    tiles = (total + TILE - 1) // TILE
    bigs = (total + BIG - 1) // BIG

    for m in range(groups):
        rows = pl.ds(pl.multiple_of(starts[m], 16), cap)
        xs[rows, :] = stage[m, 0:cap, :]
        meta = stage[m, cap : cap + META, 0:128].astype(F32)
        ids = meta[0:1, 0:cap] * 256.0 + meta[1:2, 0:cap]
        nxt = jnp.sum(jnp.where(eye_c == eye_r + 1, ids, 0.0), 1, keepdims=True)
        tid[rows, :] = nxt
        live[rows, :] = jnp.where(place < sizes[m] - 1, 1.0, 0.0)
    tail = pl.ds(pl.multiple_of(place_now, 16), TILE + 16)
    xs[tail, :] = jnp.zeros((TILE + 16, D), BF)

    def tile_at(t):
        return pl.multiple_of(off + t * TILE, 64)

    def big_rows(t):
        return pl.ds(pl.multiple_of(off + t * BIG, 64), BIG)

    def each_tile(body):
        def step(t, carry):
            body(tile_at(t), pl.ds(tile_at(t), TILE))
            return carry

        lax.fori_loop(0, tiles, step, 0)

    def each_big(body, pieces):
        def step(i, carry):
            t = i // pieces
            c = i - t * pieces
            body(big_rows(t), c)
            return carry

        lax.fori_loop(0, bigs * pieces, step, 0)

    @each_tile
    def _(base, rows):
        x = xs[rows, :].astype(F32)
        mean = jnp.mean(x, 1, keepdims=True)
        centered = x - mean
        r = lax.rsqrt(jnp.mean(centered * centered, 1, keepdims=True) + 1e-5)
        nb[rows, :] = (centered * r).astype(BF)
        rstd[rows, :] = r

    def columns_at(c, width):
        return pl.ds(pl.multiple_of(c * width, width), width)

    @functools.partial(each_big, pieces=chunks // wide_step)
    def _(rows, c):
        parts = [c * wide_step + j for j in range(wide_step)]

        @pl.when(rows.start == off)
        def _():
            for part in parts:
                wcopy(part).wait()

        cols = [columns_at(part, chunk) for part in parts]
        pres = [dot(nb[rows, :], wp[:, col], 1, 0) for col in cols]
        for col, pre in zip(cols, pres):
            sg = sigmoid(pre)
            act = pre * sg
            proj[rows, col] = act.astype(BF)
            dsil[rows, col] = (sg + act * (1.0 - sg)).astype(BF)

    keys = TILE + cap

    def labels(pos, dead):
        label = jnp.zeros(pos.shape, jnp.int32)
        inside = jnp.zeros(pos.shape, jnp.int32)
        for m in range(groups):
            after = pos >= starts[m]
            label = label + jnp.where(after, 1, 0)
            inside = jnp.where(after & (pos < starts[m] + sizes[m]), 1, inside)
        return jnp.where(inside > 0, label, dead)

    def allowed_at(base):
        q_pos = base + lax.broadcasted_iota(jnp.int32, (TILE, 1), 0)
        k_pos = base - cap + lax.broadcasted_iota(jnp.int32, (1, keys), 1)
        return (labels(q_pos, -2) == labels(k_pos, -1)) & (k_pos <= q_pos)

    def head(ref, rows, part, e):
        return ref[rows, part * HD + e * hs : part * HD + (e + 1) * hs]

    wide0 = pl.ds(0, cap)
    proj[wide0, :] = jnp.zeros((cap, 4 * HD), BF)

    @each_tile
    def _(base, rows):
        wide = pl.ds(pl.multiple_of(base - cap, 64), keys)
        allowed = allowed_at(base)
        for e0 in range(0, HEADS, 4):
            es = range(e0, e0 + 4)
            scores = [
                dot(head(proj, rows, 2, e), head(proj, wide, 3, e), 1, 1) * scale for e in es
            ]
            ws = [jnp.where(allowed, s * sigmoid(s), 0.0).astype(BF) for s in scores]
            mixed = [dot(w, head(proj, wide, 1, e), 1, 0) for w, e in zip(ws, es)]
            for e, value in zip(es, mixed):
                mix[rows, e * hs : (e + 1) * hs] = value

    @each_tile
    def _(base, rows):
        mixed = mix[rows, :]
        centered = mixed - jnp.mean(mixed, 1, keepdims=True)
        r2 = lax.rsqrt(jnp.mean(centered * centered, 1, keepdims=True) + 1e-5)
        att = centered * r2
        mix[rows, :] = att
        r2s[rows, :] = r2
        gdm[rows, :] = (att * proj[rows, 0:HD].astype(F32)).astype(BF)

    wocopy.wait()

    @functools.partial(each_big, pieces=D // width)
    def _(rows, c):
        cols = columns_at(c, width)
        out[rows, cols] = xs[rows, cols].astype(F32) + dot(gdm[rows, :], wo[:, cols], 1, 0)

    def target_rows(base):
        ext = xs[pl.ds(base, TILE + 16), :].astype(F32)
        tgt = pltpu.roll(ext, TILE + 15, 0)[0:TILE, :]
        return tgt, lax.rsqrt(jnp.sum(tgt * tgt, 1, keepdims=True) + 1e-6)

    @each_tile
    def _(base, rows):
        o = out[rows, :]
        ro = lax.rsqrt(jnp.sum(o * o, 1, keepdims=True) + 1e-6)
        gdm[rows, :] = (o * ro).astype(BF)
        tgt, rt = target_rows(base)
        poss[rows, :] = jnp.sum(o * tgt, 1, keepdims=True) * ro * rt

    for copy in pcopies:
        copy.wait()
    pool_ids = []
    for k in range(columns):
        raw = pstage[k, 0:count, :].astype(F32)
        inv = lax.rsqrt(jnp.sum(raw * raw, 1, keepdims=True) + 1e-6)
        upool[k * count : (k + 1) * count, :] = (raw * inv).astype(BF)
        meta = pstage[k, count : count + META, 0:128].astype(F32)
        pool_ids.append(meta[0:1, 0:count] * 256.0 + meta[1:2, 0:count])
    pool_ids = jnp.concatenate(pool_ids, 1)

    def clear(t, carry):
        gdm[pl.ds(tile_at(t), TILE), :] = jnp.zeros((TILE, D), BF)
        return carry

    lax.fori_loop(tiles, bigs * (BIG // TILE), clear, 0)
    dk[0:pool_size, :] = jnp.zeros((pool_size, D), F32)

    @functools.partial(each_big, pieces=1)
    def _(rows, c):
        low = gdm[rows, :]
        logits = dot(low, upool[...], 1, 1) * inv_temp
        scored = live[rows, :] > 0.5
        kept = scored & (pool_ids != tid[rows, :])
        others = jnp.where(kept, jnp.exp(logits), 0.0)
        pos = poss[rows, :] * inv_temp
        own = jnp.exp(pos)
        totals = own + jnp.sum(others, 1, keepdims=True)
        tid[rows, :] = jnp.where(scored, jnp.log(totals) - pos, 0.0)
        live[rows, :] = jnp.where(scored, (own / totals - 1.0) * inv_temp, 0.0)
        prob = jnp.where(kept, others / totals, 0.0).astype(BF)
        probs[rows, :] = prob
        dk[0:pool_size, :] += dot(prob, low, 0, 0)

    for k in range(columns):
        part = dk[k * count : (k + 1) * count, :] * inv_temp
        pstage[k, 0:count, :] = part.astype(BF)
        pcopies[k] = pltpu.make_async_copy(
            pstage.at[k, pl.ds(0, count), :], pool_out[k], hsem.at[groups + k]
        )
        pcopies[k].start()

    @each_tile
    def _(base, rows):
        o, coef = out[rows, :], live[rows, :]
        ro = lax.rsqrt(jnp.sum(o * o, 1, keepdims=True) + 1e-6)
        tgt, rt = target_rows(base)
        gu = dot(probs[rows, :], upool[...], 1, 0) * inv_temp + (coef * rt) * tgt
        og = jnp.sum(o * gu, 1, keepdims=True)
        gout = ro * gu - o * (ro * ro * ro * og)
        out[rows, :] = gout
        gdm[rows, :] = gout.astype(BF)
        cosine = poss[rows, :]
        xs[rows, :] = (
            (rt * coef * ro) * o - tgt * (rt * rt * coef * cosine)
        ).astype(BF)

    @functools.partial(each_big, pieces=HD // width)
    def _(rows, c):
        dk[rows, columns_at(c, width)] = dot(gdm[rows, :], wo[columns_at(c, width), :], 1, 1)

    gdm[wide0, :] = jnp.zeros((cap, HD), BF)

    @each_tile
    def _(base, rows):
        dg, att = dk[rows, :], mix[rows, :]
        dsil[rows, 0:HD] = (dg * att * dsil[rows, 0:HD].astype(F32)).astype(BF)
        da = dg * proj[rows, 0:HD].astype(F32)
        mean_a = jnp.mean(da, 1, keepdims=True)
        mean_b = jnp.mean(da * att, 1, keepdims=True)
        gdm[rows, :] = (r2s[rows, :] * (da - mean_a - att * mean_b)).astype(BF)

    @each_tile
    def _(base, rows):
        low_half = pl.ds(pl.multiple_of(base - cap, 64), cap)
        wide = pl.ds(pl.multiple_of(base - cap, 64), keys)
        allowed = allowed_at(base)
        for e0 in range(0, HEADS, back_heads):
            es = range(e0, e0 + back_heads)
            scores = [
                dot(head(proj, rows, 2, e), head(proj, wide, 3, e), 1, 1) * scale for e in es
            ]
            dws = [dot(head(gdm, rows, 0, e), head(proj, wide, 1, e), 1, 1) for e in es]
            ws, dss = [], []
            for score, dw in zip(scores, dws):
                sg = sigmoid(score)
                act = score * sg
                ws.append(jnp.where(allowed, act, 0.0).astype(BF))
                slope = (sg + act * (1.0 - sg)) * scale
                dss.append(jnp.where(allowed, dw * slope, 0.0).astype(BF))
            dqs = [dot(ds, head(proj, wide, 3, e), 1, 0) for ds, e in zip(dss, es)]
            dks = [dot(ds, head(proj, rows, 2, e), 0, 0) for ds, e in zip(dss, es)]
            dvs = [dot(w, head(gdm, rows, 0, e), 0, 0) for w, e in zip(ws, es)]
            for e, dq, dkk, dv in zip(es, dqs, dks, dvs):
                cols = slice(2 * HD + e * hs, 2 * HD + (e + 1) * hs)
                dsil[rows, cols] = (dq * dsil[rows, cols].astype(F32)).astype(BF)
                cols = slice(e * hs, (e + 1) * hs)
                for ref, value in ((dk, dkk), (mix, dv)):
                    ref[low_half, cols] += value[0:cap, :]
                    ref[rows, cols] = value[cap:keys, :]

    @each_tile
    def _(base, rows):
        for part, ref in ((1, mix), (3, dk)):
            cols = slice(part * HD, (part + 1) * HD)
            dsil[rows, cols] = (ref[rows, :] * dsil[rows, cols].astype(F32)).astype(BF)

    @functools.partial(each_big, pieces=D // width)
    def _(rows, c):
        mix[rows, columns_at(c, width)] = dot(dsil[rows, :], wp[columns_at(c, width), :], 1, 1)

    @each_tile
    def _(base, rows):
        dn, n = mix[rows, :], nb[rows, :].astype(F32)
        mean_a = jnp.mean(dn, 1, keepdims=True)
        mean_b = jnp.mean(dn * n, 1, keepdims=True)
        out[rows, :] = out[rows, :] + rstd[rows, :] * (dn - mean_a - n * mean_b)

    ocopies = []
    for m in range(groups):
        rows = pl.ds(pl.multiple_of(starts[m], 16), cap)
        nxt = pltpu.roll(xs[rows, :].astype(F32), 1, 0)
        grad = out[rows, :] + jnp.where(place == 0, 0.0, nxt)
        stage[m, 0:cap, :] = jnp.where(place < sizes[m], grad, 0.0).astype(BF)
        column = jnp.where(place < sizes[m], tid[rows, :], 0.0)
        line = jnp.sum(jnp.where(eye_c == eye_r, column, 0.0), 0, keepdims=True)
        stage[m, cap : cap + META, 0:128] = meta_rows([line], cap)
        ocopies.append(pltpu.make_async_copy(stage.at[m], hist_out[m], hsem.at[m]))
        ocopies[-1].start()
    for copy in ocopies + pcopies:
        copy.wait()


def final_kernel(groups, columns, cap, count, owners, rows_line, *refs):
    hist = refs[:groups]
    pools = refs[groups : groups + columns]
    picked = refs[groups + columns]
    grad_out, loss_out = refs[groups + columns + 1 :]
    block, me = my_place(groups, columns)
    total = pools[0][...].astype(F32)
    for k in range(1, columns):
        total = total + pools[k][...].astype(F32)
    raw = picked[0:count, :].astype(F32)
    inv = lax.rsqrt(jnp.sum(raw * raw, 1, keepdims=True) + 1e-6)
    own = inv * total - raw * (
        inv * inv * inv * jnp.sum(raw * total, 1, keepdims=True)
    )
    high = own.astype(BF)
    both = jnp.concatenate([high, (own - high.astype(F32)).astype(BF)], 0)
    picks = jnp.concatenate([rows_line[...]] * 2, 1)
    row = lax.broadcasted_iota(jnp.int32, (cap, 2 * count), 0)
    line = lax.broadcasted_iota(jnp.int32, (groups, cap), 0)
    losses = jnp.zeros((groups, cap), F32)
    for d in range(groups):
        h = history_at(owners, owner_at(me ^ d, block, groups), groups)
        start = pl.multiple_of(h * cap, cap)
        chosen = (row + start == picks).astype(BF)
        extra = dot(chosen, both, 1, 0)
        grad_out[pl.ds(start, cap), :] = (hist[d][0:cap, :].astype(F32) + extra).astype(BF)
        meta = hist[d][cap : cap + META, 0:128].astype(F32)
        losses = jnp.where(line == h, meta[0:1, 0:cap], losses)
    loss_out[...] = losses.astype(BF)


def spec(space):
    return pl.BlockSpec(memory_space=space)


def shape(*dims):
    return jax.ShapeDtypeStruct(dims, BF)


def per_device(actions, item_ids, lengths, owners, neg_rows, w_proj, w_out):
    slots, cap, D = actions.shape
    groups, columns = lax.axis_size("grp"), lax.axis_size("neg")
    count = neg_rows.shape[0]
    HD = w_out.shape[0]
    assert slots == groups
    flat = actions.reshape(slots * cap, D)
    rows_line = neg_rows.reshape(1, count)

    packed = pl.pallas_call(
        functools.partial(pack_kernel, groups, columns, cap),
        out_shape=[shape(cap + META, D)] * groups + [shape(count + META, D)],
        in_specs=[spec(SMEM)] * 2 + [spec(VMEM)] * 3,
        out_specs=[spec(VMEM)] * (groups + 1),
        name="pack",
    )(owners, lengths, flat, item_ids, rows_line)
    hist, picked = packed[:groups], packed[groups]

    def xor_pairs(d):
        return [
            (b * groups + p, b * groups + (p ^ d))
            for b in range(columns)
            for p in range(groups)
        ]

    def pool_pairs(k):
        return [
            (o * columns + n, b * groups + slot_of(o, b, groups))
            for o in range(groups)
            for n, b in ((n, (n + k) % columns) for n in range(columns))
        ]

    order = sorted(range(1, groups), key=lambda d: (-d))

    def exchange(parts):
        got = {0: parts[0]}
        for d in order:
            got[d] = lax.ppermute(parts[d], AXES, xor_pairs(d))
        return [got[d] for d in range(groups)]

    pool_got = [lax.ppermute(picked, AXES, pool_pairs(k)) for k in range(columns)]
    recv = exchange(hist)

    live_rows = groups * cap
    R = cap + max(pl.cdiv(live_rows, BIG) * BIG, live_rows + TILE + 16)
    pool_size = columns * count
    vm = pltpu.VMEM
    results = pl.pallas_call(
        functools.partial(main_kernel, groups, columns, cap, count),
        out_shape=[shape(cap + META, D)] * groups + [shape(count, D)] * columns,
        in_specs=[spec(ANY)] * (groups + columns + 2),
        out_specs=[spec(ANY)] * (groups + columns),
        scratch_shapes=[
            vm((D, 4 * HD), BF), vm((HD, D), BF),
            vm((groups, cap + META, D), BF), vm((columns, count + META, D), BF),
            vm((R, D), BF), vm((R, D), BF),
            vm((R, 4 * HD), BF), vm((R, 4 * HD), BF),
            vm((R, HD), F32), vm((R, D), F32), vm((R, HD), F32), vm((R, HD), BF),
            vm((pool_size, D), BF), vm((R, pool_size), BF),
            vm((R, 1), F32), vm((R, 1), F32), vm((R, 1), F32),
            vm((R, 1), F32), vm((R, 1), F32),
            pltpu.SemaphoreType.DMA((4 * HD // 256 + 1,)),
            pltpu.SemaphoreType.DMA((groups + columns,)),
        ],
        compiler_params=pltpu.CompilerParams(vmem_limit_bytes=67043328),
        cost_estimate=pl.CostEstimate(
            flops=10**10, bytes_accessed=15 * 10**6, transcendentals=10**6
        ),
        name="layer",
    )(*recv, *pool_got, w_proj, w_out)
    back = exchange(results[:groups])

    pool_back = [
        lax.ppermute(results[groups + k], AXES, [(b, a) for a, b in pool_pairs(k)])
        for k in range(columns)
    ]
    grads, losses = pl.pallas_call(
        functools.partial(final_kernel, groups, columns, cap, count),
        out_shape=[shape(slots * cap, D), shape(slots, cap)],
        in_specs=[spec(SMEM)] + [spec(VMEM)] * (groups + columns + 2),
        out_specs=[spec(VMEM)] * 2,
        name="finish",
    )(owners, rows_line, *back, *pool_back, picked)
    return grads.reshape(slots, cap, D), losses


def solution(mesh):
    whole = P(AXES)
    return jax.shard_map(
        per_device,
        mesh=mesh,
        in_specs=(whole,) * 5 + (P(), P()),
        out_specs=(whole, whole),
        check_vma=False,
    )
```

```python
import functools

import jax
import jax.numpy as jnp
from jax import lax
from jax.experimental import pallas as pl
from jax.experimental.pallas import tpu as pltpu
from jax.sharding import PartitionSpec as P

HEADS = 8
TEMP = 0.05
TILE = 128
BIG = 384
META = 8
AXES = ("grp", "neg")
BF = jnp.bfloat16
F32 = jnp.float32
VMEM = pltpu.VMEM
SMEM = pltpu.SMEM
ANY = pl.ANY


def dot(a, b, ca, cb):
    return lax.dot_general(a, b, (((ca,), (cb,)), ((), ())), preferred_element_type=F32)


def slot_of(owner, block, groups):
    return ((owner % 2) * (groups // 2) + owner // 2) ^ (2 * (block % 2))


def owner_at(slot, block, groups):
    slot = slot ^ (2 * lax.rem(block, 2))
    half = groups // 2
    return lax.rem(slot, half) * 2 + slot // half


def my_place(groups, columns):
    flat = lax.axis_index("grp") * columns + lax.axis_index("neg")
    return lax.div(flat, groups), lax.rem(flat, groups)


def meta_rows(rows, cap):
    line = lax.broadcasted_iota(jnp.int32, (META, cap), 0)
    block = jnp.zeros((META, cap), F32)
    for index, row in enumerate(rows):
        block = jnp.where(line == index, row, block)
    if cap < 128:
        block = jnp.concatenate([block, jnp.zeros((META, 128 - cap), F32)], 1)
    return block.astype(BF)


def history_at(owners_ref, owner, slots):
    found = jnp.int32(0)
    for h in range(slots):
        found = jnp.where(owners_ref[h] == owner, jnp.int32(h), found)
    return found


def pack_kernel(groups, columns, cap, owners, lengths, acts, ids, rows_line, *outs):
    hist, pool = outs[:groups], outs[groups]
    block, me = my_place(groups, columns)
    for d in range(groups):
        h = history_at(owners, owner_at(me ^ d, block, groups), groups)
        start = pl.multiple_of(h * cap, cap)
        hist[d][0:cap, :] = acts[pl.ds(start, cap), :]
        line = ids[pl.ds(h, 1), :]
        high, low = (line >> 8).astype(F32), (line & 255).astype(F32)
        hist[d][cap : cap + META, 0:128] = meta_rows(
            [high, low, lengths[h].astype(F32)], cap
        )
    count = rows_line.shape[1]
    picks = rows_line[...]
    row = lax.broadcasted_iota(jnp.int32, (groups * cap, count), 0)
    pool[0:count, :] = dot((row == picks).astype(BF), acts[...], 0, 0).astype(BF)
    shift = cap.bit_length() - 1
    place = lax.broadcasted_iota(jnp.int32, (cap, count), 0)
    within = (place == (picks & (cap - 1))).astype(BF)
    all_ids = ids[...]
    slot = lax.broadcasted_iota(jnp.int32, (groups, count), 0) == (picks >> shift)
    parts = []
    for part in (all_ids >> 8, all_ids & 255):
        table = dot(part.astype(F32).astype(BF), within, 1, 0)
        parts.append(jnp.sum(jnp.where(slot, table, 0.0), 0, keepdims=True))
    pool[count : count + META, 0:128] = meta_rows(parts, count)


def sigmoid(x):
    return 0.5 * jnp.tanh(0.5 * x) + 0.5


def main_kernel(direct, groups, columns, cap, count, *refs):
    hist_in = refs[:groups]
    pool_in = refs[groups : groups + columns]
    wp_hbm, wo_hbm = refs[groups + columns : groups + columns + 2]
    outs = refs[groups + columns + 2 :][: groups + columns]
    hist_out, pool_out = outs[:groups], outs[groups:]
    (
        wp, wo, stage, pstage, xs, nb, proj, dsil, mix, out, dk, gdm,
        upool, probs, tid, live, rstd, r2s, poss, wsem, hsem,
    ) = refs[2 * (groups + columns) + 2 :]
    D = xs.shape[1]
    HD = wo.shape[0]
    hs = HD // HEADS
    scale = hs ** -0.5
    pool_size = columns * count
    off = cap
    chunk = 256
    chunks = 4 * HD // chunk
    roomy = xs.shape[0] <= 1024
    wide_step, width, back_heads = (4, D, HEADS) if roomy else (1, chunk, 2)
    inv_temp = 1.0 / TEMP

    def wcopy(c):
        cols = pl.ds(pl.multiple_of(c * chunk, chunk), chunk)
        return pltpu.make_async_copy(wp_hbm.at[:, cols], wp.at[:, cols], wsem.at[c])

    wocopy = pltpu.make_async_copy(wo_hbm, wo, wsem.at[chunks])
    if direct:
        got, sent = hist_in, hist_out
        pool_got, pool_sent = pool_in, pool_out
    else:
        got = sent = [stage.at[m] for m in range(groups)]
        pool_got = [pstage.at[k] for k in range(columns)]
        pool_sent = [pstage.at[k, pl.ds(0, count), :] for k in range(columns)]
    hcopies = [] if direct else [
        pltpu.make_async_copy(hist_in[m], stage.at[m], hsem.at[m]) for m in range(groups)
    ]
    pcopies = [] if direct else [
        pltpu.make_async_copy(pool_in[k], pstage.at[k], hsem.at[groups + k])
        for k in range(columns)
    ]
    for copy in hcopies:
        copy.start()
    for c in range(chunks):
        wcopy(c).start()
    for copy in pcopies:
        copy.start()
    wocopy.start()
    live[...] = jnp.zeros_like(live)
    for copy in hcopies:
        copy.wait()

    eye_r = lax.broadcasted_iota(jnp.int32, (cap, cap), 0)
    eye_c = lax.broadcasted_iota(jnp.int32, (cap, cap), 1)
    place = lax.broadcasted_iota(jnp.int32, (cap, 1), 0)
    starts, sizes = [], []
    place_now = jnp.int32(off)
    for m in range(groups):
        meta = got[m][cap : cap + META, 0:128].astype(F32)
        n = jnp.max(meta[2:3, :]).astype(jnp.int32)
        starts.append(place_now)
        sizes.append(n)
        place_now = place_now + ((n + 15) // 16) * 16
    total = place_now - off
    tiles = (total + TILE - 1) // TILE
    bigs = (total + BIG - 1) // BIG

    for m in range(groups):
        rows = pl.ds(pl.multiple_of(starts[m], 16), cap)
        xs[rows, :] = got[m][0:cap, :]
        meta = got[m][cap : cap + META, 0:128].astype(F32)
        ids = meta[0:1, 0:cap] * 256.0 + meta[1:2, 0:cap]
        nxt = jnp.sum(jnp.where(eye_c == eye_r + 1, ids, 0.0), 1, keepdims=True)
        tid[rows, :] = nxt
        live[rows, :] = jnp.where(place < sizes[m] - 1, 1.0, 0.0)
    tail = pl.ds(pl.multiple_of(place_now, 16), TILE + 16)
    xs[tail, :] = jnp.zeros((TILE + 16, D), BF)

    def tile_at(t):
        return pl.multiple_of(off + t * TILE, 64)

    def big_rows(t):
        return pl.ds(pl.multiple_of(off + t * BIG, 64), BIG)

    def each_tile(body):
        def step(t, carry):
            body(tile_at(t), pl.ds(tile_at(t), TILE))
            return carry

        lax.fori_loop(0, tiles, step, 0)

    def each_big(body, pieces):
        def step(i, carry):
            t = i // pieces
            c = i - t * pieces
            body(big_rows(t), c)
            return carry

        lax.fori_loop(0, bigs * pieces, step, 0)

    @each_tile
    def _(base, rows):
        x = xs[rows, :].astype(F32)
        mean = jnp.mean(x, 1, keepdims=True)
        centered = x - mean
        r = lax.rsqrt(jnp.mean(centered * centered, 1, keepdims=True) + 1e-5)
        nb[rows, :] = (centered * r).astype(BF)
        rstd[rows, :] = r

    def columns_at(c, width):
        return pl.ds(pl.multiple_of(c * width, width), width)

    @functools.partial(each_big, pieces=chunks // wide_step)
    def _(rows, c):
        parts = [c * wide_step + j for j in range(wide_step)]

        @pl.when(rows.start == off)
        def _():
            for part in parts:
                wcopy(part).wait()

        cols = [columns_at(part, chunk) for part in parts]
        pres = [dot(nb[rows, :], wp[:, col], 1, 0) for col in cols]
        for col, pre in zip(cols, pres):
            sg = sigmoid(pre)
            act = pre * sg
            proj[rows, col] = act.astype(BF)
            dsil[rows, col] = (sg + act * (1.0 - sg)).astype(BF)

    keys = TILE + cap

    def labels(pos, dead):
        label = jnp.zeros(pos.shape, jnp.int32)
        inside = jnp.zeros(pos.shape, jnp.int32)
        for m in range(groups):
            after = pos >= starts[m]
            label = label + jnp.where(after, 1, 0)
            inside = jnp.where(after & (pos < starts[m] + sizes[m]), 1, inside)
        return jnp.where(inside > 0, label, dead)

    def allowed_at(base):
        q_pos = base + lax.broadcasted_iota(jnp.int32, (TILE, 1), 0)
        k_pos = base - cap + lax.broadcasted_iota(jnp.int32, (1, keys), 1)
        return (labels(q_pos, -2) == labels(k_pos, -1)) & (k_pos <= q_pos)

    def head(ref, rows, part, e):
        return ref[rows, part * HD + e * hs : part * HD + (e + 1) * hs]

    wide0 = pl.ds(0, cap)
    proj[wide0, :] = jnp.zeros((cap, 4 * HD), BF)

    @each_tile
    def _(base, rows):
        wide = pl.ds(pl.multiple_of(base - cap, 64), keys)
        allowed = allowed_at(base)
        for e0 in range(0, HEADS, 4):
            es = range(e0, e0 + 4)
            scores = [
                dot(head(proj, rows, 2, e), head(proj, wide, 3, e), 1, 1) * scale for e in es
            ]
            ws = [jnp.where(allowed, s * sigmoid(s), 0.0).astype(BF) for s in scores]
            mixed = [dot(w, head(proj, wide, 1, e), 1, 0) for w, e in zip(ws, es)]
            for e, value in zip(es, mixed):
                mix[rows, e * hs : (e + 1) * hs] = value

    @each_tile
    def _(base, rows):
        mixed = mix[rows, :]
        centered = mixed - jnp.mean(mixed, 1, keepdims=True)
        r2 = lax.rsqrt(jnp.mean(centered * centered, 1, keepdims=True) + 1e-5)
        att = centered * r2
        mix[rows, :] = att
        r2s[rows, :] = r2
        gdm[rows, :] = (att * proj[rows, 0:HD].astype(F32)).astype(BF)

    wocopy.wait()

    @functools.partial(each_big, pieces=D // width)
    def _(rows, c):
        cols = columns_at(c, width)
        out[rows, cols] = xs[rows, cols].astype(F32) + dot(gdm[rows, :], wo[:, cols], 1, 0)

    def target_rows(base):
        ext = xs[pl.ds(base, TILE + 16), :].astype(F32)
        tgt = pltpu.roll(ext, TILE + 15, 0)[0:TILE, :]
        return tgt, lax.rsqrt(jnp.sum(tgt * tgt, 1, keepdims=True) + 1e-6)

    @each_tile
    def _(base, rows):
        o = out[rows, :]
        ro = lax.rsqrt(jnp.sum(o * o, 1, keepdims=True) + 1e-6)
        gdm[rows, :] = (o * ro).astype(BF)
        tgt, rt = target_rows(base)
        poss[rows, :] = jnp.sum(o * tgt, 1, keepdims=True) * ro * rt

    for copy in pcopies:
        copy.wait()
    pool_ids = []
    for k in range(columns):
        raw = pool_got[k][0:count, :].astype(F32)
        inv = lax.rsqrt(jnp.sum(raw * raw, 1, keepdims=True) + 1e-6)
        upool[k * count : (k + 1) * count, :] = (raw * inv).astype(BF)
        meta = pool_got[k][count : count + META, 0:128].astype(F32)
        pool_ids.append(meta[0:1, 0:count] * 256.0 + meta[1:2, 0:count])
    pool_ids = jnp.concatenate(pool_ids, 1)

    def clear(t, carry):
        gdm[pl.ds(tile_at(t), TILE), :] = jnp.zeros((TILE, D), BF)
        return carry

    lax.fori_loop(tiles, bigs * (BIG // TILE), clear, 0)
    dk[0:pool_size, :] = jnp.zeros((pool_size, D), F32)

    @functools.partial(each_big, pieces=1)
    def _(rows, c):
        low = gdm[rows, :]
        logits = dot(low, upool[...], 1, 1) * inv_temp
        scored = live[rows, :] > 0.5
        kept = scored & (pool_ids != tid[rows, :])
        others = jnp.where(kept, jnp.exp(logits), 0.0)
        pos = poss[rows, :] * inv_temp
        own = jnp.exp(pos)
        totals = own + jnp.sum(others, 1, keepdims=True)
        tid[rows, :] = jnp.where(scored, jnp.log(totals) - pos, 0.0)
        live[rows, :] = jnp.where(scored, (own / totals - 1.0) * inv_temp, 0.0)
        prob = jnp.where(kept, others / totals, 0.0).astype(BF)
        probs[rows, :] = prob
        dk[0:pool_size, :] += dot(prob, low, 0, 0)

    for k in range(columns):
        part = dk[k * count : (k + 1) * count, :] * inv_temp
        pool_sent[k][...] = part.astype(BF)
        if not direct:
            pcopies[k] = pltpu.make_async_copy(
                pool_sent[k], pool_out[k], hsem.at[groups + k]
            )
            pcopies[k].start()

    @each_tile
    def _(base, rows):
        o, coef = out[rows, :], live[rows, :]
        ro = lax.rsqrt(jnp.sum(o * o, 1, keepdims=True) + 1e-6)
        tgt, rt = target_rows(base)
        gu = dot(probs[rows, :], upool[...], 1, 0) * inv_temp + (coef * rt) * tgt
        og = jnp.sum(o * gu, 1, keepdims=True)
        gout = ro * gu - o * (ro * ro * ro * og)
        out[rows, :] = gout
        gdm[rows, :] = gout.astype(BF)
        cosine = poss[rows, :]
        xs[rows, :] = (
            (rt * coef * ro) * o - tgt * (rt * rt * coef * cosine)
        ).astype(BF)

    @functools.partial(each_big, pieces=HD // width)
    def _(rows, c):
        dk[rows, columns_at(c, width)] = dot(gdm[rows, :], wo[columns_at(c, width), :], 1, 1)

    gdm[wide0, :] = jnp.zeros((cap, HD), BF)

    @each_tile
    def _(base, rows):
        dg, att = dk[rows, :], mix[rows, :]
        dsil[rows, 0:HD] = (dg * att * dsil[rows, 0:HD].astype(F32)).astype(BF)
        da = dg * proj[rows, 0:HD].astype(F32)
        mean_a = jnp.mean(da, 1, keepdims=True)
        mean_b = jnp.mean(da * att, 1, keepdims=True)
        gdm[rows, :] = (r2s[rows, :] * (da - mean_a - att * mean_b)).astype(BF)

    @each_tile
    def _(base, rows):
        low_half = pl.ds(pl.multiple_of(base - cap, 64), cap)
        wide = pl.ds(pl.multiple_of(base - cap, 64), keys)
        allowed = allowed_at(base)
        for e0 in range(0, HEADS, back_heads):
            es = range(e0, e0 + back_heads)
            scores = [
                dot(head(proj, rows, 2, e), head(proj, wide, 3, e), 1, 1) * scale for e in es
            ]
            dws = [dot(head(gdm, rows, 0, e), head(proj, wide, 1, e), 1, 1) for e in es]
            ws, dss = [], []
            for score, dw in zip(scores, dws):
                sg = sigmoid(score)
                act = score * sg
                ws.append(jnp.where(allowed, act, 0.0).astype(BF))
                slope = (sg + act * (1.0 - sg)) * scale
                dss.append(jnp.where(allowed, dw * slope, 0.0).astype(BF))
            dqs = [dot(ds, head(proj, wide, 3, e), 1, 0) for ds, e in zip(dss, es)]
            dks = [dot(ds, head(proj, rows, 2, e), 0, 0) for ds, e in zip(dss, es)]
            dvs = [dot(w, head(gdm, rows, 0, e), 0, 0) for w, e in zip(ws, es)]
            for e, dq, dkk, dv in zip(es, dqs, dks, dvs):
                cols = slice(2 * HD + e * hs, 2 * HD + (e + 1) * hs)
                dsil[rows, cols] = (dq * dsil[rows, cols].astype(F32)).astype(BF)
                cols = slice(e * hs, (e + 1) * hs)
                for ref, value in ((dk, dkk), (mix, dv)):
                    ref[low_half, cols] += value[0:cap, :]
                    ref[rows, cols] = value[cap:keys, :]

    @each_tile
    def _(base, rows):
        for part, ref in ((1, mix), (3, dk)):
            cols = slice(part * HD, (part + 1) * HD)
            dsil[rows, cols] = (ref[rows, :] * dsil[rows, cols].astype(F32)).astype(BF)

    @functools.partial(each_big, pieces=D // width)
    def _(rows, c):
        mix[rows, columns_at(c, width)] = dot(dsil[rows, :], wp[columns_at(c, width), :], 1, 1)

    @each_tile
    def _(base, rows):
        dn, n = mix[rows, :], nb[rows, :].astype(F32)
        mean_a = jnp.mean(dn, 1, keepdims=True)
        mean_b = jnp.mean(dn * n, 1, keepdims=True)
        out[rows, :] = out[rows, :] + rstd[rows, :] * (dn - mean_a - n * mean_b)

    ocopies = []
    for m in range(groups):
        rows = pl.ds(pl.multiple_of(starts[m], 16), cap)
        nxt = pltpu.roll(xs[rows, :].astype(F32), 1, 0)
        grad = out[rows, :] + jnp.where(place == 0, 0.0, nxt)
        sent[m][0:cap, :] = jnp.where(place < sizes[m], grad, 0.0).astype(BF)
        column = jnp.where(place < sizes[m], tid[rows, :], 0.0)
        line = jnp.sum(jnp.where(eye_c == eye_r, column, 0.0), 0, keepdims=True)
        sent[m][cap : cap + META, 0:128] = meta_rows([line], cap)
        if not direct:
            ocopies.append(pltpu.make_async_copy(sent[m], hist_out[m], hsem.at[m]))
            ocopies[-1].start()
    for copy in ocopies + pcopies:
        copy.wait()


def final_kernel(groups, columns, cap, count, owners, rows_line, *refs):
    hist = refs[:groups]
    pools = refs[groups : groups + columns]
    picked = refs[groups + columns]
    grad_out, loss_out = refs[groups + columns + 1 :]
    block, me = my_place(groups, columns)
    total = pools[0][...].astype(F32)
    for k in range(1, columns):
        total = total + pools[k][...].astype(F32)
    raw = picked[0:count, :].astype(F32)
    inv = lax.rsqrt(jnp.sum(raw * raw, 1, keepdims=True) + 1e-6)
    own = inv * total - raw * (
        inv * inv * inv * jnp.sum(raw * total, 1, keepdims=True)
    )
    high = own.astype(BF)
    both = jnp.concatenate([high, (own - high.astype(F32)).astype(BF)], 0)
    picks = jnp.concatenate([rows_line[...]] * 2, 1)
    row = lax.broadcasted_iota(jnp.int32, (cap, 2 * count), 0)
    line = lax.broadcasted_iota(jnp.int32, (groups, cap), 0)
    losses = jnp.zeros((groups, cap), F32)
    for d in range(groups):
        h = history_at(owners, owner_at(me ^ d, block, groups), groups)
        start = pl.multiple_of(h * cap, cap)
        chosen = (row + start == picks).astype(BF)
        extra = dot(chosen, both, 1, 0)
        grad_out[pl.ds(start, cap), :] = (hist[d][0:cap, :].astype(F32) + extra).astype(BF)
        meta = hist[d][cap : cap + META, 0:128].astype(F32)
        losses = jnp.where(line == h, meta[0:1, 0:cap], losses)
    loss_out[...] = losses.astype(BF)


def spec(space):
    return pl.BlockSpec(memory_space=space)


def shape(*dims):
    return jax.ShapeDtypeStruct(dims, BF)


def per_device(actions, item_ids, lengths, owners, neg_rows, w_proj, w_out):
    slots, cap, D = actions.shape
    groups, columns = lax.axis_size("grp"), lax.axis_size("neg")
    count = neg_rows.shape[0]
    HD = w_out.shape[0]
    assert slots == groups
    flat = actions.reshape(slots * cap, D)
    rows_line = neg_rows.reshape(1, count)
    vm = pltpu.VMEM
    roomy = slots * cap <= 512

    def place(dims):
        return vm(dims, BF) if roomy else shape(*dims)

    def keep(parts):
        if not roomy:
            return list(parts)
        return [pltpu.with_memory_space_constraint(part, pltpu.VMEM) for part in parts]


    packed = pl.pallas_call(
        functools.partial(pack_kernel, groups, columns, cap),
        out_shape=[place((cap + META, D))] * groups + [place((count + META, D))],
        in_specs=[spec(SMEM)] * 2 + [spec(VMEM)] * 3,
        out_specs=[spec(VMEM)] * (groups + 1),
        name="pack",
    )(owners, lengths, flat, item_ids, rows_line)
    hist, picked = packed[:groups], packed[groups]

    def xor_pairs(d):
        return [
            (b * groups + p, b * groups + (p ^ d))
            for b in range(columns)
            for p in range(groups)
        ]

    def pool_pairs(k):
        return [
            (o * columns + n, b * groups + slot_of(o, b, groups))
            for o in range(groups)
            for n, b in ((n, (n + k) % columns) for n in range(columns))
        ]

    order = sorted(range(1, groups), key=lambda d: (-d))

    def exchange(parts):
        got = {0: parts[0]}
        for d in order:
            got[d] = lax.ppermute(parts[d], AXES, xor_pairs(d))
        return [got[d] for d in range(groups)]

    pool_got = [lax.ppermute(picked, AXES, pool_pairs(k)) for k in range(columns)]
    recv = exchange(hist)

    live_rows = groups * cap
    R = cap + max(pl.cdiv(live_rows, BIG) * BIG, live_rows + TILE + 16)
    pool_size = columns * count
    results = pl.pallas_call(
        functools.partial(main_kernel, roomy, groups, columns, cap, count),
        out_shape=[place((cap + META, D))] * groups + [place((count, D))] * columns,
        in_specs=[spec(VMEM if roomy else ANY)] * (groups + columns) + [spec(ANY)] * 2,
        out_specs=[spec(VMEM if roomy else ANY)] * (groups + columns),
        scratch_shapes=[
            vm((D, 4 * HD), BF), vm((HD, D), BF),
            vm((1 if roomy else groups, cap + META, D), BF),
            vm((1 if roomy else columns, count + META, D), BF),
            vm((R, D), BF), vm((R, D), BF),
            vm((R, 4 * HD), BF), vm((R, 4 * HD), BF),
            vm((R, HD), F32), vm((R, D), F32), vm((R, HD), F32), vm((R, HD), BF),
            vm((pool_size, D), BF), vm((R, pool_size), BF),
            vm((R, 1), F32), vm((R, 1), F32), vm((R, 1), F32),
            vm((R, 1), F32), vm((R, 1), F32),
            pltpu.SemaphoreType.DMA((4 * HD // 256 + 1,)),
            pltpu.SemaphoreType.DMA((groups + columns,)),
        ],
        compiler_params=pltpu.CompilerParams(vmem_limit_bytes=(52 * 2**20 if roomy else 67043328)),
        cost_estimate=pl.CostEstimate(
            flops=10**10, bytes_accessed=15 * 10**6, transcendentals=10**6
        ),
        name="layer",
    )(*keep(recv), *keep(pool_got), w_proj, w_out)
    back = exchange(results[:groups])

    pool_back = [
        lax.ppermute(results[groups + k], AXES, [(b, a) for a, b in pool_pairs(k)])
        for k in range(columns)
    ]
    grads, losses = pl.pallas_call(
        functools.partial(final_kernel, groups, columns, cap, count),
        out_shape=[shape(slots * cap, D), shape(slots, cap)],
        in_specs=[spec(SMEM)] + [spec(VMEM)] * (groups + columns + 2),
        out_specs=[spec(VMEM)] * 2,
        name="finish",
    )(owners, rows_line, *keep([*back, *pool_back, picked]))
    return grads.reshape(slots, cap, D), losses


def solution(mesh):
    whole = P(AXES)
    return jax.shard_map(
        per_device,
        mesh=mesh,
        in_specs=(whole,) * 5 + (P(), P()),
        out_specs=(whole, whole),
        check_vma=False,
    )
```

```python
import functools

import jax
import jax.numpy as jnp
from jax import lax
from jax.experimental import pallas as pl
from jax.experimental.pallas import tpu as pltpu
from jax.sharding import PartitionSpec as P

HEADS = 8
TEMP = 0.05
TILE = 128
BIG = 384
META = 8
AXES = ("grp", "neg")
BF = jnp.bfloat16
F32 = jnp.float32
VMEM = pltpu.VMEM
SMEM = pltpu.SMEM
ANY = pl.ANY


def dot(a, b, ca, cb):
    return lax.dot_general(a, b, (((ca,), (cb,)), ((), ())), preferred_element_type=F32)


def slot_of(owner, block, groups):
    return ((owner % 2) * (groups // 2) + owner // 2) ^ (2 * (block % 2))


def owner_at(slot, block, groups):
    slot = slot ^ (2 * lax.rem(block, 2))
    half = groups // 2
    return lax.rem(slot, half) * 2 + slot // half


def my_place(groups, columns):
    flat = lax.axis_index("grp") * columns + lax.axis_index("neg")
    return lax.div(flat, groups), lax.rem(flat, groups)


def meta_rows(rows, cap):
    line = lax.broadcasted_iota(jnp.int32, (META, cap), 0)
    block = jnp.zeros((META, cap), F32)
    for index, row in enumerate(rows):
        block = jnp.where(line == index, row, block)
    if cap < 128:
        block = jnp.concatenate([block, jnp.zeros((META, 128 - cap), F32)], 1)
    return block.astype(BF)


def history_at(owners_ref, owner, slots):
    found = jnp.int32(0)
    for h in range(slots):
        found = jnp.where(owners_ref[h] == owner, jnp.int32(h), found)
    return found


def pack_kernel(groups, columns, cap, owners, lengths, acts, ids, rows_line, *outs):
    hist, pool = outs[:groups], outs[groups]
    block, me = my_place(groups, columns)
    for d in range(groups):
        h = history_at(owners, owner_at(me ^ d, block, groups), groups)
        start = pl.multiple_of(h * cap, cap)
        hist[d][0:cap, :] = acts[pl.ds(start, cap), :]
        line = ids[pl.ds(h, 1), :]
        high, low = (line >> 8).astype(F32), (line & 255).astype(F32)
        hist[d][cap : cap + META, 0:128] = meta_rows(
            [high, low, lengths[h].astype(F32)], cap
        )
    count = rows_line.shape[1]
    picks = rows_line[...]
    row = lax.broadcasted_iota(jnp.int32, (groups * cap, count), 0)
    pool[0:count, :] = dot((row == picks).astype(BF), acts[...], 0, 0).astype(BF)
    shift = cap.bit_length() - 1
    place = lax.broadcasted_iota(jnp.int32, (cap, count), 0)
    within = (place == (picks & (cap - 1))).astype(BF)
    all_ids = ids[...]
    slot = lax.broadcasted_iota(jnp.int32, (groups, count), 0) == (picks >> shift)
    parts = []
    for part in (all_ids >> 8, all_ids & 255):
        table = dot(part.astype(F32).astype(BF), within, 1, 0)
        parts.append(jnp.sum(jnp.where(slot, table, 0.0), 0, keepdims=True))
    pool[count : count + META, 0:128] = meta_rows(parts, count)


def sigmoid(x):
    return 0.5 * jnp.tanh(0.5 * x) + 0.5


def main_kernel(direct, groups, columns, cap, count, *refs):
    hist_in = refs[:groups]
    pool_in = refs[groups : groups + columns]
    wp_hbm, wo_hbm = refs[groups + columns : groups + columns + 2]
    outs = refs[groups + columns + 2 :][: groups + columns]
    hist_out, pool_out = outs[:groups], outs[groups:]
    (
        wp, wo, stage, pstage, xs, nb, proj, dsil, mix, out, dk, gdm,
        upool, probs, tid, live, rstd, r2s, poss, wsem, hsem,
    ) = refs[2 * (groups + columns) + 2 :]
    D = xs.shape[1]
    HD = wo.shape[0]
    hs = HD // HEADS
    scale = hs ** -0.5
    pool_size = columns * count
    off = cap
    chunk = 256
    chunks = 4 * HD // chunk
    roomy = xs.shape[0] <= 1024
    wide_step, width, back_heads = (4, D, HEADS) if roomy else (1, chunk, 2)
    fore_heads = HEADS if roomy else 4
    inv_temp = 1.0 / TEMP

    def wcopy(c):
        cols = pl.ds(pl.multiple_of(c * chunk, chunk), chunk)
        return pltpu.make_async_copy(wp_hbm.at[:, cols], wp.at[:, cols], wsem.at[c])

    wocopy = pltpu.make_async_copy(wo_hbm, wo, wsem.at[chunks])
    if direct:
        got, sent = hist_in, hist_out
        pool_got, pool_sent = pool_in, pool_out
    else:
        got = sent = [stage.at[m] for m in range(groups)]
        pool_got = [pstage.at[k] for k in range(columns)]
        pool_sent = [pstage.at[k, pl.ds(0, count), :] for k in range(columns)]
    hcopies = [] if direct else [
        pltpu.make_async_copy(hist_in[m], stage.at[m], hsem.at[m]) for m in range(groups)
    ]
    pcopies = [] if direct else [
        pltpu.make_async_copy(pool_in[k], pstage.at[k], hsem.at[groups + k])
        for k in range(columns)
    ]
    for copy in hcopies:
        copy.start()
    for c in range(chunks):
        wcopy(c).start()
    for copy in pcopies:
        copy.start()
    wocopy.start()
    live[...] = jnp.zeros_like(live)
    for copy in hcopies:
        copy.wait()

    eye_r = lax.broadcasted_iota(jnp.int32, (cap, cap), 0)
    eye_c = lax.broadcasted_iota(jnp.int32, (cap, cap), 1)
    place = lax.broadcasted_iota(jnp.int32, (cap, 1), 0)
    starts, sizes = [], []
    place_now = jnp.int32(off)
    for m in range(groups):
        meta = got[m][cap : cap + META, 0:128].astype(F32)
        n = jnp.max(meta[2:3, :]).astype(jnp.int32)
        starts.append(place_now)
        sizes.append(n)
        place_now = place_now + ((n + 15) // 16) * 16
    total = place_now - off
    tiles = (total + TILE - 1) // TILE
    bigs = (total + BIG - 1) // BIG

    for m in range(groups):
        rows = pl.ds(pl.multiple_of(starts[m], 16), cap)
        xs[rows, :] = got[m][0:cap, :]
        meta = got[m][cap : cap + META, 0:128].astype(F32)
        ids = meta[0:1, 0:cap] * 256.0 + meta[1:2, 0:cap]
        nxt = jnp.sum(jnp.where(eye_c == eye_r + 1, ids, 0.0), 1, keepdims=True)
        tid[rows, :] = nxt
        live[rows, :] = jnp.where(place < sizes[m] - 1, 1.0, 0.0)
    tail = pl.ds(pl.multiple_of(place_now, 16), TILE + 16)
    xs[tail, :] = jnp.zeros((TILE + 16, D), BF)

    def tile_at(t):
        return pl.multiple_of(off + t * TILE, 64)

    def big_rows(t):
        return pl.ds(pl.multiple_of(off + t * BIG, 64), BIG)

    def each_tile(body):
        def step(t, carry):
            body(tile_at(t), pl.ds(tile_at(t), TILE))
            return carry

        lax.fori_loop(0, tiles, step, 0)

    def each_big(body, pieces):
        def step(i, carry):
            t = i // pieces
            c = i - t * pieces
            body(big_rows(t), c)
            return carry

        lax.fori_loop(0, bigs * pieces, step, 0)

    @each_tile
    def _(base, rows):
        x = xs[rows, :].astype(F32)
        mean = jnp.mean(x, 1, keepdims=True)
        centered = x - mean
        r = lax.rsqrt(jnp.mean(centered * centered, 1, keepdims=True) + 1e-5)
        nb[rows, :] = (centered * r).astype(BF)
        rstd[rows, :] = r

    def columns_at(c, width):
        return pl.ds(pl.multiple_of(c * width, width), width)

    @functools.partial(each_big, pieces=chunks // wide_step)
    def _(rows, c):
        parts = [c * wide_step + j for j in range(wide_step)]

        @pl.when(rows.start == off)
        def _():
            for part in parts:
                wcopy(part).wait()

        cols = [columns_at(part, chunk) for part in parts]
        pres = [dot(nb[rows, :], wp[:, col], 1, 0) for col in cols]
        for col, pre in zip(cols, pres):
            sg = sigmoid(pre)
            act = pre * sg
            proj[rows, col] = act.astype(BF)
            dsil[rows, col] = (sg + act * (1.0 - sg)).astype(BF)

    keys = TILE + cap

    def labels(pos, dead):
        label = jnp.zeros(pos.shape, jnp.int32)
        inside = jnp.zeros(pos.shape, jnp.int32)
        for m in range(groups):
            after = pos >= starts[m]
            label = label + jnp.where(after, 1, 0)
            inside = jnp.where(after & (pos < starts[m] + sizes[m]), 1, inside)
        return jnp.where(inside > 0, label, dead)

    def allowed_at(base):
        q_pos = base + lax.broadcasted_iota(jnp.int32, (TILE, 1), 0)
        k_pos = base - cap + lax.broadcasted_iota(jnp.int32, (1, keys), 1)
        return (labels(q_pos, -2) == labels(k_pos, -1)) & (k_pos <= q_pos)

    def head(ref, rows, part, e):
        return ref[rows, part * HD + e * hs : part * HD + (e + 1) * hs]

    wide0 = pl.ds(0, cap)
    proj[wide0, :] = jnp.zeros((cap, 4 * HD), BF)

    @each_tile
    def _(base, rows):
        wide = pl.ds(pl.multiple_of(base - cap, 64), keys)
        allowed = allowed_at(base)
        for e0 in range(0, HEADS, fore_heads):
            es = range(e0, e0 + fore_heads)
            scores = [
                dot(head(proj, rows, 2, e), head(proj, wide, 3, e), 1, 1) * scale for e in es
            ]
            ws = [jnp.where(allowed, s * sigmoid(s), 0.0).astype(BF) for s in scores]
            mixed = [dot(w, head(proj, wide, 1, e), 1, 0) for w, e in zip(ws, es)]
            for e, value in zip(es, mixed):
                mix[rows, e * hs : (e + 1) * hs] = value

    @each_tile
    def _(base, rows):
        mixed = mix[rows, :]
        centered = mixed - jnp.mean(mixed, 1, keepdims=True)
        r2 = lax.rsqrt(jnp.mean(centered * centered, 1, keepdims=True) + 1e-5)
        att = centered * r2
        mix[rows, :] = att
        r2s[rows, :] = r2
        gdm[rows, :] = (att * proj[rows, 0:HD].astype(F32)).astype(BF)

    wocopy.wait()

    @functools.partial(each_big, pieces=D // width)
    def _(rows, c):
        cols = columns_at(c, width)
        out[rows, cols] = xs[rows, cols].astype(F32) + dot(gdm[rows, :], wo[:, cols], 1, 0)

    def target_rows(base):
        ext = xs[pl.ds(base, TILE + 16), :].astype(F32)
        tgt = pltpu.roll(ext, TILE + 15, 0)[0:TILE, :]
        return tgt, lax.rsqrt(jnp.sum(tgt * tgt, 1, keepdims=True) + 1e-6)

    @each_tile
    def _(base, rows):
        o = out[rows, :]
        ro = lax.rsqrt(jnp.sum(o * o, 1, keepdims=True) + 1e-6)
        gdm[rows, :] = (o * ro).astype(BF)
        tgt, rt = target_rows(base)
        poss[rows, :] = jnp.sum(o * tgt, 1, keepdims=True) * ro * rt

    for copy in pcopies:
        copy.wait()
    pool_ids = []
    for k in range(columns):
        raw = pool_got[k][0:count, :].astype(F32)
        inv = lax.rsqrt(jnp.sum(raw * raw, 1, keepdims=True) + 1e-6)
        upool[k * count : (k + 1) * count, :] = (raw * inv).astype(BF)
        meta = pool_got[k][count : count + META, 0:128].astype(F32)
        pool_ids.append(meta[0:1, 0:count] * 256.0 + meta[1:2, 0:count])
    pool_ids = jnp.concatenate(pool_ids, 1)

    def clear(t, carry):
        gdm[pl.ds(tile_at(t), TILE), :] = jnp.zeros((TILE, D), BF)
        return carry

    lax.fori_loop(tiles, bigs * (BIG // TILE), clear, 0)
    dk[0:pool_size, :] = jnp.zeros((pool_size, D), F32)

    @functools.partial(each_big, pieces=1)
    def _(rows, c):
        low = gdm[rows, :]
        logits = dot(low, upool[...], 1, 1) * inv_temp
        scored = live[rows, :] > 0.5
        kept = scored & (pool_ids != tid[rows, :])
        others = jnp.where(kept, jnp.exp(logits), 0.0)
        pos = poss[rows, :] * inv_temp
        own = jnp.exp(pos)
        totals = own + jnp.sum(others, 1, keepdims=True)
        tid[rows, :] = jnp.where(scored, jnp.log(totals) - pos, 0.0)
        live[rows, :] = jnp.where(scored, (own / totals - 1.0) * inv_temp, 0.0)
        prob = jnp.where(kept, others / totals, 0.0).astype(BF)
        probs[rows, :] = prob
        dk[0:pool_size, :] += dot(prob, low, 0, 0)

    for k in range(columns):
        part = dk[k * count : (k + 1) * count, :] * inv_temp
        pool_sent[k][...] = part.astype(BF)
        if not direct:
            pcopies[k] = pltpu.make_async_copy(
                pool_sent[k], pool_out[k], hsem.at[groups + k]
            )
            pcopies[k].start()

    @each_tile
    def _(base, rows):
        o, coef = out[rows, :], live[rows, :]
        ro = lax.rsqrt(jnp.sum(o * o, 1, keepdims=True) + 1e-6)
        tgt, rt = target_rows(base)
        gu = dot(probs[rows, :], upool[...], 1, 0) * inv_temp + (coef * rt) * tgt
        og = jnp.sum(o * gu, 1, keepdims=True)
        gout = ro * gu - o * (ro * ro * ro * og)
        out[rows, :] = gout
        gdm[rows, :] = gout.astype(BF)
        cosine = poss[rows, :]
        xs[rows, :] = (
            (rt * coef * ro) * o - tgt * (rt * rt * coef * cosine)
        ).astype(BF)

    @functools.partial(each_big, pieces=HD // width)
    def _(rows, c):
        dk[rows, columns_at(c, width)] = dot(gdm[rows, :], wo[columns_at(c, width), :], 1, 1)

    gdm[wide0, :] = jnp.zeros((cap, HD), BF)

    @each_tile
    def _(base, rows):
        dg, att = dk[rows, :], mix[rows, :]
        dsil[rows, 0:HD] = (dg * att * dsil[rows, 0:HD].astype(F32)).astype(BF)
        da = dg * proj[rows, 0:HD].astype(F32)
        mean_a = jnp.mean(da, 1, keepdims=True)
        mean_b = jnp.mean(da * att, 1, keepdims=True)
        gdm[rows, :] = (r2s[rows, :] * (da - mean_a - att * mean_b)).astype(BF)

    @each_tile
    def _(base, rows):
        low_half = pl.ds(pl.multiple_of(base - cap, 64), cap)
        wide = pl.ds(pl.multiple_of(base - cap, 64), keys)
        allowed = allowed_at(base)
        for e0 in range(0, HEADS, back_heads):
            es = range(e0, e0 + back_heads)
            scores = [
                dot(head(proj, rows, 2, e), head(proj, wide, 3, e), 1, 1) * scale for e in es
            ]
            dws = [dot(head(gdm, rows, 0, e), head(proj, wide, 1, e), 1, 1) for e in es]
            ws, dss = [], []
            for score, dw in zip(scores, dws):
                sg = sigmoid(score)
                act = score * sg
                ws.append(jnp.where(allowed, act, 0.0).astype(BF))
                slope = (sg + act * (1.0 - sg)) * scale
                dss.append(jnp.where(allowed, dw * slope, 0.0).astype(BF))
            dqs = [dot(ds, head(proj, wide, 3, e), 1, 0) for ds, e in zip(dss, es)]
            dks = [dot(ds, head(proj, rows, 2, e), 0, 0) for ds, e in zip(dss, es)]
            dvs = [dot(w, head(gdm, rows, 0, e), 0, 0) for w, e in zip(ws, es)]
            for e, dq, dkk, dv in zip(es, dqs, dks, dvs):
                cols = slice(2 * HD + e * hs, 2 * HD + (e + 1) * hs)
                dsil[rows, cols] = (dq * dsil[rows, cols].astype(F32)).astype(BF)
                cols = slice(e * hs, (e + 1) * hs)
                for ref, value in ((dk, dkk), (mix, dv)):
                    ref[low_half, cols] += value[0:cap, :]
                    ref[rows, cols] = value[cap:keys, :]

    @each_tile
    def _(base, rows):
        for part, ref in ((1, mix), (3, dk)):
            cols = slice(part * HD, (part + 1) * HD)
            dsil[rows, cols] = (ref[rows, :] * dsil[rows, cols].astype(F32)).astype(BF)

    @functools.partial(each_big, pieces=D // width)
    def _(rows, c):
        mix[rows, columns_at(c, width)] = dot(dsil[rows, :], wp[columns_at(c, width), :], 1, 1)

    @each_tile
    def _(base, rows):
        dn, n = mix[rows, :], nb[rows, :].astype(F32)
        mean_a = jnp.mean(dn, 1, keepdims=True)
        mean_b = jnp.mean(dn * n, 1, keepdims=True)
        out[rows, :] = out[rows, :] + rstd[rows, :] * (dn - mean_a - n * mean_b)

    ocopies = []
    for m in range(groups):
        rows = pl.ds(pl.multiple_of(starts[m], 16), cap)
        nxt = pltpu.roll(xs[rows, :].astype(F32), 1, 0)
        grad = out[rows, :] + jnp.where(place == 0, 0.0, nxt)
        sent[m][0:cap, :] = jnp.where(place < sizes[m], grad, 0.0).astype(BF)
        column = jnp.where(place < sizes[m], tid[rows, :], 0.0)
        line = jnp.sum(jnp.where(eye_c == eye_r, column, 0.0), 0, keepdims=True)
        sent[m][cap : cap + META, 0:128] = meta_rows([line], cap)
        if not direct:
            ocopies.append(pltpu.make_async_copy(sent[m], hist_out[m], hsem.at[m]))
            ocopies[-1].start()
    for copy in ocopies + pcopies:
        copy.wait()


def final_kernel(groups, columns, cap, count, owners, rows_line, *refs):
    hist = refs[:groups]
    pools = refs[groups : groups + columns]
    picked = refs[groups + columns]
    grad_out, loss_out = refs[groups + columns + 1 :]
    block, me = my_place(groups, columns)
    total = pools[0][...].astype(F32)
    for k in range(1, columns):
        total = total + pools[k][...].astype(F32)
    raw = picked[0:count, :].astype(F32)
    inv = lax.rsqrt(jnp.sum(raw * raw, 1, keepdims=True) + 1e-6)
    own = inv * total - raw * (
        inv * inv * inv * jnp.sum(raw * total, 1, keepdims=True)
    )
    high = own.astype(BF)
    both = jnp.concatenate([high, (own - high.astype(F32)).astype(BF)], 0)
    picks = jnp.concatenate([rows_line[...]] * 2, 1)
    row = lax.broadcasted_iota(jnp.int32, (cap, 2 * count), 0)
    line = lax.broadcasted_iota(jnp.int32, (groups, cap), 0)
    losses = jnp.zeros((groups, cap), F32)
    for d in range(groups):
        h = history_at(owners, owner_at(me ^ d, block, groups), groups)
        start = pl.multiple_of(h * cap, cap)
        chosen = (row + start == picks).astype(BF)
        extra = dot(chosen, both, 1, 0)
        grad_out[pl.ds(start, cap), :] = (hist[d][0:cap, :].astype(F32) + extra).astype(BF)
        meta = hist[d][cap : cap + META, 0:128].astype(F32)
        losses = jnp.where(line == h, meta[0:1, 0:cap], losses)
    loss_out[...] = losses.astype(BF)


def spec(space):
    return pl.BlockSpec(memory_space=space)


def shape(*dims):
    return jax.ShapeDtypeStruct(dims, BF)


def per_device(actions, item_ids, lengths, owners, neg_rows, w_proj, w_out):
    slots, cap, D = actions.shape
    groups, columns = lax.axis_size("grp"), lax.axis_size("neg")
    count = neg_rows.shape[0]
    HD = w_out.shape[0]
    assert slots == groups
    flat = actions.reshape(slots * cap, D)
    rows_line = neg_rows.reshape(1, count)
    vm = pltpu.VMEM
    roomy = slots * cap <= 512

    def place(dims):
        return vm(dims, BF) if roomy else shape(*dims)

    def keep(parts):
        if not roomy:
            return list(parts)
        return [pltpu.with_memory_space_constraint(part, pltpu.VMEM) for part in parts]


    packed = pl.pallas_call(
        functools.partial(pack_kernel, groups, columns, cap),
        out_shape=[place((cap + META, D))] * groups + [place((count + META, D))],
        in_specs=[spec(SMEM)] * 2 + [spec(VMEM)] * 3,
        out_specs=[spec(VMEM)] * (groups + 1),
        name="pack",
    )(owners, lengths, flat, item_ids, rows_line)
    hist, picked = packed[:groups], packed[groups]

    def xor_pairs(d):
        return [
            (b * groups + p, b * groups + (p ^ d))
            for b in range(columns)
            for p in range(groups)
        ]

    def pool_pairs(k):
        return [
            (o * columns + n, b * groups + slot_of(o, b, groups))
            for o in range(groups)
            for n, b in ((n, (n + k) % columns) for n in range(columns))
        ]

    order = sorted(range(1, groups), key=lambda d: (-d))

    def exchange(parts):
        got = {0: parts[0]}
        for d in order:
            got[d] = lax.ppermute(parts[d], AXES, xor_pairs(d))
        return [got[d] for d in range(groups)]

    pool_got = [lax.ppermute(picked, AXES, pool_pairs(k)) for k in range(columns)]
    recv = exchange(hist)

    live_rows = groups * cap
    R = cap + max(pl.cdiv(live_rows, BIG) * BIG, live_rows + TILE + 16)
    pool_size = columns * count
    results = pl.pallas_call(
        functools.partial(main_kernel, roomy, groups, columns, cap, count),
        out_shape=[place((cap + META, D))] * groups + [place((count, D))] * columns,
        in_specs=[spec(VMEM if roomy else ANY)] * (groups + columns) + [spec(ANY)] * 2,
        out_specs=[spec(VMEM if roomy else ANY)] * (groups + columns),
        scratch_shapes=[
            vm((D, 4 * HD), BF), vm((HD, D), BF),
            vm((1 if roomy else groups, cap + META, D), BF),
            vm((1 if roomy else columns, count + META, D), BF),
            vm((R, D), BF), vm((R, D), BF),
            vm((R, 4 * HD), BF), vm((R, 4 * HD), BF),
            vm((R, HD), F32), vm((R, D), F32), vm((R, HD), F32), vm((R, HD), BF),
            vm((pool_size, D), BF), vm((R, pool_size), BF),
            vm((R, 1), F32), vm((R, 1), F32), vm((R, 1), F32),
            vm((R, 1), F32), vm((R, 1), F32),
            pltpu.SemaphoreType.DMA((4 * HD // 256 + 1,)),
            pltpu.SemaphoreType.DMA((groups + columns,)),
        ],
        compiler_params=pltpu.CompilerParams(vmem_limit_bytes=(52 * 2**20 if roomy else 67043328)),
        cost_estimate=pl.CostEstimate(
            flops=10**10, bytes_accessed=15 * 10**6, transcendentals=10**6
        ),
        name="layer",
    )(*keep(recv), *keep(pool_got), w_proj, w_out)
    back = exchange(results[:groups])

    pool_back = [
        lax.ppermute(results[groups + k], AXES, [(b, a) for a, b in pool_pairs(k)])
        for k in range(columns)
    ]
    grads, losses = pl.pallas_call(
        functools.partial(final_kernel, groups, columns, cap, count),
        out_shape=[shape(slots * cap, D), shape(slots, cap)],
        in_specs=[spec(SMEM)] + [spec(VMEM)] * (groups + columns + 2),
        out_specs=[spec(VMEM)] * 2,
        name="finish",
    )(owners, rows_line, *keep([*back, *pool_back, picked]))
    return grads.reshape(slots, cap, D), losses


def solution(mesh):
    whole = P(AXES)
    return jax.shard_map(
        per_device,
        mesh=mesh,
        in_specs=(whole,) * 5 + (P(), P()),
        out_specs=(whole, whole),
        check_vma=False,
    )
```
